32 devices in a mesh: dp: 1 (over z), gz: 4 (over y), gy: 4 (over x), gx: 2 (over core).
Axes of the slice: x: 4, y: 4, z: 1, core: 2. Of those that a mesh axis runs over, the one named last changes fastest.
The devices are a block of a 4x4x8 slice.
Arguments:
- volume: bfloat16 [32, 96, 192, 192], P('dp', 'gx', 'gy', 'gz')
- cot_out: bfloat16 [32, 96, 192, 192], P('dp', 'gx', 'gy', 'gz')
- filter_taps: float32 [3, 3, 11], replicated
- w_mix: bfloat16 [3, 32, 32], replicated
- b_mix: float32 [3, 32], replicated
Outputs:
- output 1: bfloat16 [32, 96, 192, 192], P('dp', 'gx', 'gy', 'gz')
- output 2: float32 [3, 32, 32], P('dp')
- output 3: float32 [3, 32], P('dp')
All inputs are finite; a program needn't handle non-finite values.
Results may differ from the reference program's by a relative error of at most 0.0144.
Values are sent between devices in bfloat16 or wider.
A program may use at most 768 MiB of HBM per device.

```python
import jax
import jax.numpy as jnp
from jax import lax

CHANNELS = 32
NUM_TAPS = 11
LAYERS = 3
GRID_X = 96
GRID_Y = 192
GRID_Z = 192
HALF_TAPS = (NUM_TAPS - 1) // 2
TWO_PI = 6.283185307179586


def smooth_field(key):
    keys = jax.random.split(key, 4)
    num_modes = 4
    wave_len = NUM_TAPS * jax.random.uniform(keys[0], (3, num_modes), jnp.float32, 1.0, 3.0)
    phases = jax.random.uniform(keys[1], (3, num_modes), jnp.float32, 0.0, TWO_PI)
    mode_amp = 1.4 * jax.random.normal(keys[2], (CHANNELS, num_modes), jnp.float32)
    profiles = [jnp.cos(TWO_PI * jnp.arange(extent, dtype=jnp.float32)[None, :] / wave_len[axis][:, None] + phases[axis][:, None]) for axis, extent in enumerate((GRID_X, GRID_Y, GRID_Z))]
    field = jnp.einsum('cm,mx,my,mz->cxyz', mode_amp, profiles[0], profiles[1], profiles[2])
    noise = jax.random.normal(keys[3], field.shape, jnp.float32)
    return field + 0.3 * noise


def setup_inputs(seed: int = 0, part: int = 0) -> dict:
    base_key = jax.random.key(seed)
    shared_key, part_root = jax.random.split(base_key)
    vol_key, cot_key = jax.random.split(jax.random.fold_in(part_root, part), 2)
    tap_key, mix_key, bias_key = jax.random.split(shared_key, 3)
    volume = smooth_field(vol_key).astype(jnp.bfloat16)
    cot_out = smooth_field(cot_key).astype(jnp.bfloat16)
    raw_taps = jax.random.uniform(tap_key, (LAYERS, 3, NUM_TAPS), jnp.float32, 0.5, 1.5)
    filter_taps = (raw_taps / jnp.sum(raw_taps, axis=-1, keepdims=True)).astype(jnp.bfloat16).astype(jnp.float32)
    w_mix = (jax.random.normal(mix_key, (LAYERS, CHANNELS, CHANNELS), jnp.float32) * CHANNELS ** -0.5).astype(jnp.bfloat16)
    b_mix = 0.5 * jax.random.normal(bias_key, (LAYERS, CHANNELS), jnp.float32)
    return {'volume': volume, 'cot_out': cot_out, 'filter_taps': filter_taps, 'w_mix': w_mix, 'b_mix': b_mix}


def filter_line(values, taps, axis):
    length = values.shape[axis]
    pad_widths = [(0, 0)] * values.ndim
    pad_widths[axis] = (HALF_TAPS, HALF_TAPS)
    padded = jnp.pad(values, pad_widths)
    total = jnp.zeros(values.shape, jnp.float32)
    for tap_idx in range(NUM_TAPS):
        total = total + taps[tap_idx] * lax.slice_in_dim(padded, tap_idx, tap_idx + length, axis=axis)
    return total


def filter_three(channel, taps3):
    first = filter_line(channel.astype(jnp.float32), taps3[0], 0).astype(jnp.bfloat16)
    second = filter_line(first.astype(jnp.float32), taps3[1], 1).astype(jnp.bfloat16)
    return filter_line(second.astype(jnp.float32), taps3[2], 2).astype(jnp.bfloat16)


def filter_three_back(channel, taps3):
    first = filter_line(channel.astype(jnp.float32), taps3[2][::-1], 2).astype(jnp.bfloat16)
    second = filter_line(first.astype(jnp.float32), taps3[1][::-1], 1).astype(jnp.bfloat16)
    return filter_line(second.astype(jnp.float32), taps3[0][::-1], 0)


def gelu_exact(pre_act):
    return jax.nn.gelu(pre_act, approximate=False)


def reference(volume, cot_out, filter_taps, w_mix, b_mix):
    def forward_layer(vol_cur, layer):
        taps3, w_layer, b_layer = layer
        filtered = lax.map(lambda channel: filter_three(channel, taps3), vol_cur)
        pre_act = jnp.einsum('cd,cxyz->dxyz', w_layer.astype(jnp.float32), filtered.astype(jnp.float32)) + b_layer[:, None, None, None]
        vol_next = (vol_cur.astype(jnp.float32) + gelu_exact(pre_act)).astype(jnp.bfloat16)
        return vol_next, filtered

    _, filtered_all = lax.scan(forward_layer, volume, (filter_taps, w_mix, b_mix))

    def backward_layer(grad_next, layer):
        taps3, w_layer, b_layer, filtered = layer
        pre_act = jnp.einsum('cd,cxyz->dxyz', w_layer.astype(jnp.float32), filtered.astype(jnp.float32)) + b_layer[:, None, None, None]
        _, pullback = jax.vjp(gelu_exact, pre_act)
        scaled = pullback(grad_next.astype(jnp.float32))[0]
        scaled_b = scaled.astype(jnp.bfloat16).astype(jnp.float32)
        grad_b = jnp.sum(scaled, axis=(1, 2, 3))
        grad_w = jnp.einsum('cxyz,dxyz->cd', filtered.astype(jnp.float32), scaled_b)
        mixed_back = jnp.einsum('cd,dxyz->cxyz', w_layer.astype(jnp.float32), scaled_b).astype(jnp.bfloat16)
        spread = lax.map(lambda channel: filter_three_back(channel, taps3), mixed_back)
        grad_prev = (grad_next.astype(jnp.float32) + spread).astype(jnp.bfloat16)
        return grad_prev, (grad_w, grad_b)

    grad_volume, (grad_w_mix, grad_bias) = lax.scan(backward_layer, cot_out, (filter_taps, w_mix, b_mix, filtered_all), reverse=True)
    return grad_volume, grad_w_mix, grad_bias
```

```python
import functools

import jax
import jax.numpy as jnp
from jax import lax
from jax.experimental import pallas as pl
from jax.experimental.pallas import tpu as pltpu
from jax.sharding import PartitionSpec as P

MESH = pl.DeviceIdType.MESH
TILE = 256
ROWS = 16
INV_SQRT2 = 0.7071067811865476
INV_SQRT_2PI = 0.3989422804014327
F32 = jnp.float32
BF16 = jnp.bfloat16


def banded(taps, index, keep):
    num_taps = taps.shape[1]
    out = jnp.zeros((taps.shape[0],) + index.shape, F32)
    for t in range(num_taps):
        out = jnp.where((index == t) & keep, taps[:, t][:, None, None], out)
    return out.astype(BF16)


def grid2(rows, cols):
    return jnp.arange(rows)[:, None], jnp.arange(cols)[None, :]


def x_matrix(taps, half, chans):
    r, n = grid2(3 * TILE, TILE)
    index = r // chans - TILE // chans - n // chans + half
    return banded(taps, index, r % chans == n % chans)


def y_matrix(taps, half, side):
    group = ROWS - 2 * half
    r, k = grid2(group * ROWS, ROWS * ROWS)
    yi, zi = k // ROWS, k % ROWS
    main = banded(taps, yi - r // ROWS, r % ROWS == zi)
    if side is None:
        return main
    r, k = grid2(2 * ROWS, ROWS * ROWS)
    sub, q = r // ROWS, r % ROWS
    yo = sub * (group // 2) + q // half
    zo = q % half + (0 if side == 0 else ROWS - half)
    extra = banded(taps, yi - yo, (zo == zi) & (q < (group // 2) * half))
    return jnp.concatenate([main, extra], axis=1)


def z_matrix(taps, half, ysub, nz):
    r, k = grid2(ysub * nz, ysub * nz + 2 * ROWS)
    yo, zo = r // nz, r % nz
    is_main = k < ysub * nz
    q = (k - ysub * nz) % ROWS
    low = k < ysub * nz + ROWS
    yi = jnp.where(is_main, k // nz, q // half)
    zi = jnp.where(is_main, k % nz, jnp.where(low, q % half - half, nz + q % half))
    keep = (yi == yo) & (is_main | (q < ysub * half))
    return banded(taps, zi - zo + half, keep)


def pick_matrix(half, ysub, nz):
    r, k = grid2(2 * ROWS, ysub * nz)
    q = r % ROWS
    zo = q % half + jnp.where(r < ROWS, 0, nz - half)
    hit = (k // nz == q // half) & (k % nz == zo) & (q < ysub * half)
    return hit.astype(BF16)


def dims(shape, half):
    ny, nz, lanes = shape
    group = ROWS - 2 * half
    return ny, nz, lanes, lanes // TILE, group, group // 2


def lane_ds(tile):
    return pl.ds(pl.multiple_of(tile * TILE, TILE), TILE)


class Links:
    def __init__(self, sizes):
        self.sizes = sizes
        self.pos = {name: lax.axis_index(name) for name in ('gx', 'gy', 'gz')}

    def barrier(self):
        sem = pltpu.get_barrier_semaphore()
        count = 1
        pl.semaphore_signal(sem, inc=1, device_id={'gx': 1 - self.pos['gx']}, device_id_type=MESH)
        for name in ('gy', 'gz'):
            size = self.sizes[name]
            for step in (1, size - 1):
                pl.semaphore_signal(sem, inc=1, device_id={name: lax.rem(self.pos[name] + step, size)}, device_id_type=MESH)
                count += 1
        pl.semaphore_wait(sem, count)

    def pair(self, name, low_src, high_dst, high_src, low_dst, sems, tile):
        send, recv = sems
        pos, size = self.pos[name], self.sizes[name]
        down = pltpu.make_async_remote_copy(low_src, high_dst, send.at[0, tile], recv.at[0, tile], device_id={name: jnp.maximum(pos - 1, 0)}, device_id_type=MESH)
        up = pltpu.make_async_remote_copy(high_src, low_dst, send.at[1, tile], recv.at[1, tile], device_id={name: jnp.minimum(pos + 1, size - 1)}, device_id_type=MESH)
        return (down, pos > 0), (up, pos < size - 1)

    def start(self, flows):
        for copy, has in flows:
            pl.when(has)(copy.start)

    def wait_recv(self, flows):
        (down, has_low), (up, has_high) = flows
        pl.when(has_high)(down.wait_recv)
        pl.when(has_low)(up.wait_recv)

    def wait_send(self, flows):
        for copy, has in flows:
            pl.when(has)(copy.wait_send)

    def zero_edges(self, name, low_ref, high_ref):
        @pl.when(self.pos[name] == 0)
        def _():
            low_ref[...] = jnp.zeros_like(low_ref)

        @pl.when(self.pos[name] == self.sizes[name] - 1)
        def _():
            high_ref[...] = jnp.zeros_like(high_ref)

    def x_edge(self, ext, sems, lanes):
        send, recv = sems
        me = self.pos['gx']
        src = pl.multiple_of(lanes + me * (TILE - lanes), TILE)
        dst = pl.multiple_of(me * (lanes + TILE), TILE)
        return pltpu.make_async_remote_copy(ext.at[:, :, pl.ds(src, TILE)], ext.at[:, :, pl.ds(dst, TILE)], send, recv, device_id={'gx': 1 - me}, device_id_type=MESH)

    def zero_x(self, ext, lanes):
        start = pl.multiple_of((1 - self.pos['gx']) * 0 + self.pos['gx'] * (lanes + TILE), TILE)
        ny = ext.shape[0]

        @pl.loop(0, ny)
        def _(y):
            ext[y, :, pl.ds(start, TILE)] = jnp.zeros((ext.shape[1], TILE), ext.dtype)


def y_flows(links, buf, half, ny, sems, tile):
    cols = lane_ds(tile)
    return links.pair('gy', buf.at[pl.ds(half, half), :, cols], buf.at[pl.ds(ny + half, half), :, cols], buf.at[pl.ds(ny, half), :, cols], buf.at[pl.ds(0, half), :, cols], sems, tile)


def z_flows(links, zs, zr, sems, tile):
    cols = lane_ds(tile)
    return links.pair('gz', zs.at[0, :, :, cols], zr.at[1, :, :, cols], zs.at[1, :, :, cols], zr.at[0, :, :, cols], sems, tile)


def dot(a, b):
    return jnp.dot(a, b, preferred_element_type=F32)


def x_pass_rows(ext, wx, tile, start, count):
    nz = ext.shape[1]
    block = ext[pl.ds(start, count), :, pl.ds(pl.multiple_of(tile * TILE, TILE), 3 * TILE)]
    return dot(block.reshape(count * nz, 3 * TILE), wx[...])


def fwd_kernel(half, sizes, last, *refs):
    if last:
        (v_hbm, wx, lya, lyb, lz, wd, bias, a3_hbm, vext, a1, a2, a3, zs, zr, in_sem, out_sem, xsend, xrecv, ysend, yrecv, zsend, zrecv) = refs
    else:
        (v_hbm, wx, lya, lyb, lz, wd, bias, a3_hbm, vo_hbm, vext, a1, a2, a3, zs, zr, in_sem, out_sem, xsend, xrecv, ysend, yrecv, zsend, zrecv) = refs
    ny, nz, lanes, tiles, group, ysub = dims(v_hbm.shape, half)
    links = Links(sizes)
    me = links.pos['gx']

    def order(step):
        return step + me * (tiles - 1 - 2 * step)

    def fetch(tile):
        return pltpu.make_async_copy(v_hbm.at[:, :, lane_ds(tile)], vext.at[:, :, lane_ds(tile + 1)], in_sem.at[tile])

    edge = order(tiles - 1)
    fetch(edge).start()
    for step in range(tiles - 1):
        fetch(order(step)).start()
    links.zero_edges('gy', a1.at[pl.ds(0, half)], a1.at[pl.ds(ny + half, half)])
    links.zero_edges('gz', zr.at[0], zr.at[1])
    links.zero_x(vext, lanes)
    links.barrier()
    fetch(edge).wait()
    xcopy = links.x_edge(vext, (xsend, xrecv), lanes)
    xcopy.start()
    fetch(order(0)).wait()

    def x_phase(tile):
        count = 8 if ny % 8 == 0 else ysub
        for y in range(0, ny, count):
            out = x_pass_rows(vext, wx, tile, y, count)
            a1[pl.ds(y + half, count), :, lane_ds(tile)] = out.astype(BF16).reshape(count, nz, TILE)
        links.start(y_flows(links, a1, half, ny, (ysend, yrecv), tile))

    @pl.loop(0, tiles - 1)
    def _(step):
        @pl.when(step < tiles - 2)
        def _():
            fetch(order(step + 1)).wait()
        x_phase(order(step))

    xcopy.wait_recv()
    x_phase(edge)

    @pl.loop(0, tiles)
    def _(step):
        tile = order(step)
        cols = lane_ds(tile)
        links.wait_recv(y_flows(links, a1, half, ny, (ysend, yrecv), tile))
        for g in range(ny // group):
            for zb in range(nz // ROWS):
                side = {0: 0, nz // ROWS - 1: 1}.get(zb)
                mat = lya if side == 0 else lyb
                rhs = a1[pl.ds(g * group, ROWS), pl.ds(zb * ROWS, ROWS), cols].reshape(ROWS * ROWS, TILE)
                lhs = mat[...] if side is not None else mat[pl.ds(0, group * ROWS), :]
                out = dot(lhs, rhs).astype(BF16)
                a2[pl.ds(g * group, group), pl.ds(zb * ROWS, ROWS), cols] = out[: group * ROWS].reshape(group, ROWS, TILE)
                if side is not None:
                    zs[side, pl.ds(2 * g, 2), :, cols] = out[group * ROWS :].reshape(2, ROWS, TILE)
        links.start(z_flows(links, zs, zr, (zsend, zrecv), tile))

    xcopy.wait_send()

    def put_a3(tile):
        return pltpu.make_async_copy(a3.at[:, :, lane_ds(tile)], a3_hbm.at[:, :, lane_ds(tile)], out_sem.at[0, tile])

    def put_v(tile):
        return pltpu.make_async_copy(vext.at[:, :, lane_ds(tile + 1)], vo_hbm.at[:, :, lane_ds(tile)], out_sem.at[1, tile])

    @pl.loop(0, tiles)
    def _(step):
        tile = order(step)
        cols = lane_ds(tile)
        links.wait_recv(z_flows(links, zs, zr, (zsend, zrecv), tile))
        for g in range(ny // ysub):
            main = a2[pl.ds(g * ysub, ysub), :, cols].reshape(ysub * nz, TILE)
            rhs = jnp.concatenate([main, zr[0, g, :, cols], zr[1, g, :, cols]], axis=0)
            out = dot(lz[...], rhs).astype(BF16)
            a3[pl.ds(g * ysub, ysub), :, cols] = out.reshape(ysub, nz, TILE)
            if not last:
                pre = dot(out, wd[...]) + bias[...]
                act = 0.5 * pre * (1.0 + lax.erf(pre * INV_SQRT2))
                vcols = lane_ds(tile + 1)
                old = vext[pl.ds(g * ysub, ysub), :, vcols].astype(F32).reshape(ysub * nz, TILE)
                vext[pl.ds(g * ysub, ysub), :, vcols] = (old + act).astype(BF16).reshape(ysub, nz, TILE)
        put_a3(tile).start()
        if not last:
            put_v(tile).start()

    @pl.loop(0, tiles)
    def _(tile):
        links.wait_send(y_flows(links, a1, half, ny, (ysend, yrecv), tile))
        links.wait_send(z_flows(links, zs, zr, (zsend, zrecv), tile))
        put_a3(tile).wait()
        if not last:
            put_v(tile).wait()


def bwd_kernel(half, sizes, a3_hbm, g_hbm, wx, ly, lz, pick, wd, wt, bias, go_hbm, dw_ref, db_ref, a3, grad, sb, d3, d2, dext, zs, zr, in_sem, out_sem, xsend, xrecv, ysend, yrecv, zsend, zrecv):
    ny, nz, lanes, tiles, group, ysub = dims(g_hbm.shape, half)
    links = Links(sizes)
    me = links.pos['gx']

    def order(step):
        return (tiles - 1 - step) + me * (2 * step - tiles + 1)

    def fetch(tile):
        cols = lane_ds(tile)
        return (pltpu.make_async_copy(a3_hbm.at[:, :, cols], a3.at[:, :, cols], in_sem.at[0, tile]), pltpu.make_async_copy(g_hbm.at[:, :, cols], grad.at[:, :, cols], in_sem.at[1, tile]))

    for step in range(tiles):
        for copy in fetch(order(step)):
            copy.start()
    links.zero_edges('gy', d2.at[pl.ds(0, half)], d2.at[pl.ds(ny + half, half)])
    links.zero_edges('gz', zr.at[0], zr.at[1])
    links.zero_x(dext, lanes)
    dw_ref[...] = jnp.zeros_like(dw_ref)
    db_ref[...] = jnp.zeros_like(db_ref)
    links.barrier()

    @pl.loop(0, tiles)
    def _(step):
        tile = order(step)
        cols = lane_ds(tile)
        for copy in fetch(tile):
            copy.wait()
        for g in range(ny // ysub):
            rows = pl.ds(g * ysub, ysub)
            act = a3[rows, :, cols].reshape(ysub * nz, TILE)
            pre = dot(act, wd[...]) + bias[...]
            cot = grad[rows, :, cols].astype(F32).reshape(ysub * nz, TILE)
            slope = 0.5 + 0.5 * lax.erf(pre * INV_SQRT2) + pre * (INV_SQRT_2PI * jnp.exp(-0.5 * pre * pre))
            scaled = slope * cot
            db_ref[...] += jnp.sum(scaled.reshape(ysub * nz // 8, 8, TILE), axis=0)
            low = scaled.astype(BF16)
            sb[pl.ds(g * ysub * nz, ysub * nz), :] = low
            mixed = dot(low, wt[...]).astype(BF16)
            d3[rows, :, cols] = mixed.reshape(ysub, nz, TILE)
            planes = dot(pick[...], mixed).astype(BF16)
            zs[0, g, :, cols] = planes[:ROWS]
            zs[1, g, :, cols] = planes[ROWS:]
        links.start(z_flows(links, zs, zr, (zsend, zrecv), tile))
        acts = a3[:, :, cols].reshape(ny * nz, TILE)
        dw_ref[...] += lax.dot_general(acts, sb[...], (((0,), (0,)), ((), ())), preferred_element_type=F32)

    @pl.loop(0, tiles)
    def _(step):
        tile = order(step)
        cols = lane_ds(tile)
        links.wait_recv(z_flows(links, zs, zr, (zsend, zrecv), tile))
        for g in range(ny // ysub):
            main = d3[pl.ds(g * ysub, ysub), :, cols].reshape(ysub * nz, TILE)
            rhs = jnp.concatenate([main, zr[0, g, :, cols], zr[1, g, :, cols]], axis=0)
            out = dot(lz[...], rhs).astype(BF16)
            d2[pl.ds(g * ysub + half, ysub), :, cols] = out.reshape(ysub, nz, TILE)
        links.start(y_flows(links, d2, half, ny, (ysend, yrecv), tile))

    xcopy = links.x_edge(dext, (xsend, xrecv), lanes)

    @pl.loop(0, tiles)
    def _(step):
        tile = order(step)
        cols = lane_ds(tile)
        links.wait_recv(y_flows(links, d2, half, ny, (ysend, yrecv), tile))
        for g in range(ny // group):
            for zb in range(nz // ROWS):
                rhs = d2[pl.ds(g * group, ROWS), pl.ds(zb * ROWS, ROWS), cols].reshape(ROWS * ROWS, TILE)
                out = dot(ly[...], rhs).astype(BF16)
                dext[pl.ds(g * group, group), pl.ds(zb * ROWS, ROWS), lane_ds(tile + 1)] = out.reshape(group, ROWS, TILE)
        pl.when(step == 0)(xcopy.start)

    def put(tile):
        return pltpu.make_async_copy(grad.at[:, :, lane_ds(tile)], go_hbm.at[:, :, lane_ds(tile)], out_sem.at[tile])

    def x_phase(tile):
        cols = lane_ds(tile)
        count = 8 if ny % 8 == 0 else ysub
        for y in range(0, ny, count):
            rows = pl.ds(y, count)
            spread = x_pass_rows(dext, wx, tile, y, count)
            old = grad[rows, :, cols].astype(F32).reshape(count * nz, TILE)
            grad[rows, :, cols] = (old + spread).astype(BF16).reshape(count, nz, TILE)
        put(tile).start()

    @pl.loop(0, tiles - 1)
    def _(step):
        x_phase(order(tiles - 1 - step))

    xcopy.wait_recv()
    x_phase(order(0))
    xcopy.wait_send()

    @pl.loop(0, tiles)
    def _(tile):
        links.wait_send(y_flows(links, d2, half, ny, (ysend, yrecv), tile))
        links.wait_send(z_flows(links, zs, zr, (zsend, zrecv), tile))
        put(tile).wait()


def link_sems(tiles):
    dma = pltpu.SemaphoreType.DMA
    return [dma, dma, dma((2, tiles)), dma((2, tiles)), dma((2, tiles)), dma((2, tiles))]


def solution(mesh):
    names = ('gx', 'gy', 'gz')
    sizes = {name: mesh.shape[name] for name in names}
    vol_spec = P('dp', 'gx', 'gy', 'gz')
    any_spec = pl.BlockSpec(memory_space=pl.ANY)
    vmem_spec = pl.BlockSpec(memory_space=pltpu.VMEM)
    dma = pltpu.SemaphoreType.DMA

    def local_step(volume, cot_out, filter_taps, w_mix, b_mix):
        chans, nx, ny, nz = volume.shape
        num_layers, _, num_taps = filter_taps.shape
        half = (num_taps - 1) // 2
        lanes = nx * chans
        tiles = lanes // TILE
        reps = TILE // chans
        group = ROWS - 2 * half
        ysub = group // 2
        params = functools.partial(pltpu.CompilerParams, has_side_effects=True, vmem_limit_bytes=60 * 1024 * 1024)
        block = jax.ShapeDtypeStruct((ny, nz, lanes), BF16)
        back_taps = filter_taps[:, :, ::-1]
        wx_f = x_matrix(filter_taps[:, 0], half, chans)
        wx_b = x_matrix(back_taps[:, 0], half, chans)
        lya = y_matrix(filter_taps[:, 1], half, 0)
        lyb = y_matrix(filter_taps[:, 1], half, 1)
        ly_b = y_matrix(back_taps[:, 1], half, None)
        lz_f = z_matrix(filter_taps[:, 2], half, ysub, nz)
        lz_b = z_matrix(back_taps[:, 2], half, ysub, nz)
        pick = pick_matrix(half, ysub, nz)
        same = jnp.eye(reps, dtype=BF16)
        wd = (same[None, :, None, :, None] * w_mix[:, None, :, None, :]).reshape(num_layers, TILE, TILE)
        wt = jnp.swapaxes(wd, 1, 2)
        bias = jnp.tile(b_mix, (1, reps))[:, None, :]

        def to_dense(a):
            return jnp.transpose(a, (2, 3, 1, 0)).reshape(ny, nz, lanes)

        halo = pltpu.VMEM((2, ny // ysub, ROWS, lanes), BF16)
        full = pltpu.VMEM((ny, nz, lanes), BF16)
        tall = pltpu.VMEM((ny + 2 * half, nz, lanes), BF16)
        wide = pltpu.VMEM((ny, nz, lanes + 2 * TILE), BF16)

        cur = to_dense(volume)
        acts = []
        for layer in range(num_layers):
            last = layer + 1 == num_layers
            outs = pl.pallas_call(
                functools.partial(fwd_kernel, half, sizes, last),
                out_shape=[block] * (1 if last else 2),
                in_specs=[any_spec] + [vmem_spec] * 6,
                out_specs=[any_spec] * (1 if last else 2),
                scratch_shapes=[wide, tall, full, full, halo, halo, dma((tiles,)), dma((2, tiles))] + link_sems(tiles),
                compiler_params=params(collective_id=layer),
                name='fwd_layer',
            )(cur, wx_f[layer], lya[layer], lyb[layer], lz_f[layer], wd[layer], bias[layer])
            acts.append(outs[0])
            if not last:
                cur = outs[1]

        grad = to_dense(cot_out)
        grad_w, grad_b = [None] * num_layers, [None] * num_layers
        for layer in reversed(range(num_layers)):
            grad, dw, db = pl.pallas_call(
                functools.partial(bwd_kernel, half, sizes),
                out_shape=[block, jax.ShapeDtypeStruct((TILE, TILE), F32), jax.ShapeDtypeStruct((8, TILE), F32)],
                in_specs=[any_spec] * 2 + [vmem_spec] * 7,
                out_specs=[any_spec, vmem_spec, vmem_spec],
                scratch_shapes=[full, full, pltpu.VMEM((ny * nz, TILE), BF16), full, tall, wide, halo, halo, dma((2, tiles)), dma((tiles,))] + link_sems(tiles),
                compiler_params=params(collective_id=num_layers + layer),
                name='bwd_layer',
            )(acts[layer], grad, wx_b[layer], ly_b[layer], lz_b[layer], pick, wd[layer], wt[layer], bias[layer])
            dw4 = dw.reshape(reps, chans, reps, chans)
            grad_w[layer] = sum(dw4[i, :, i, :] for i in range(reps))
            grad_b[layer] = jnp.sum(db.reshape(8 * reps, chans), axis=0)
        grad_volume = jnp.transpose(grad.reshape(ny, nz, nx, chans), (3, 2, 0, 1))
        grad_w_sum = lax.psum(jnp.stack(grad_w), names)
        grad_b_sum = lax.psum(jnp.stack(grad_b), names)
        return grad_volume, grad_w_sum, grad_b_sum

    return jax.shard_map(local_step, mesh=mesh, in_specs=(vol_spec, vol_spec, P(), P(), P()), out_specs=(vol_spec, P('dp'), P('dp')), check_vma=False)
```

```python
import functools

import jax
import jax.numpy as jnp
import numpy as np
from jax import lax
from jax.experimental import pallas as pl
from jax.experimental.pallas import tpu as pltpu
from jax.sharding import PartitionSpec as P

MESH = pl.DeviceIdType.MESH
TILE = 256
ROWS = 16
LANE = 128
SUB = 8
VMEM_BYTES = 60 * 1024 * 1024
INV_SQRT2 = 0.7071067811865476
INV_SQRT_2PI = 0.3989422804014327
F32 = jnp.float32
BF16 = jnp.bfloat16


def valid_index(index, keep, num_taps):
    return np.where(keep & (index >= 0) & (index < num_taps), index, -1).astype(np.int32)


def grid2(rows, cols):
    return np.arange(rows)[:, None], np.arange(cols)[None, :]


def x_index(num_taps, chans):
    r, n = grid2(3 * TILE, TILE)
    index = r // chans - TILE // chans - n // chans + num_taps // 2
    return valid_index(index, r % chans == n % chans, num_taps)


def y_index(num_taps):
    half = num_taps // 2
    group = ROWS - 2 * half
    r, k = grid2(group * ROWS, ROWS * ROWS)
    yi, zi = k // ROWS, k % ROWS
    parts = [valid_index(yi - r // ROWS, r % ROWS == zi, num_taps)]
    r, k = grid2(2 * ROWS, ROWS * ROWS)
    q = r % ROWS
    yo = r // ROWS * (group // 2) + q // half
    for first in (0, ROWS - half):
        keep = (q % half + first == zi) & (q < (group // 2) * half)
        parts.append(valid_index(yi - yo, keep, num_taps))
    return np.concatenate(parts, axis=0)


def z_index(num_taps, ysub, nz):
    half = num_taps // 2
    r, k = grid2(ysub * nz, ysub * nz + 2 * ROWS)
    yo, zo = r // nz, r % nz
    is_main = k < ysub * nz
    q = (k - ysub * nz) % ROWS
    low = k < ysub * nz + ROWS
    yi = np.where(is_main, k // nz, q // half)
    zi = np.where(is_main, k % nz, np.where(low, q % half - half, nz + q % half))
    keep = (yi == yo) & (is_main | (q < ysub * half))
    return valid_index(zi - zo + half, keep, num_taps)


def pick_matrix(half, ysub, nz):
    r, k = grid2(2 * ROWS, ysub * nz)
    q = r % ROWS
    zo = q % half + np.where(r < ROWS, 0, nz - half)
    hit = (k // nz == q // half) & (k % nz == zo) & (q < ysub * half)
    return jnp.asarray(hit, BF16)


def band_kernel(taps, wmix, spread, same, xi, yi, zi, xf, xb, yf, yb, zf, zb, wd, wt):
    layers, _, num_taps = taps.shape
    reps = TILE // spread.shape[0]
    for axis, index, fwd, bwd in ((0, xi, xf, xb), (1, yi, yf, yb), (2, zi, zf, zb)):
        @pl.loop(0, index.shape[0] // ROWS)
        def _(chunk):
            rows = pl.ds(pl.multiple_of(chunk * ROWS, ROWS), ROWS)
            which = index[rows, :]
            zero = jnp.zeros(which.shape, F32)
            out = [[zero] * layers, [zero] * layers]
            for t in range(num_taps):
                hit = which == t
                for layer in range(layers):
                    out[0][layer] = jnp.where(hit, taps[layer, axis, t], out[0][layer])
                    out[1][layer] = jnp.where(hit, taps[layer, axis, num_taps - 1 - t], out[1][layer])
            for layer in range(layers):
                fwd[layer, rows, :] = out[0][layer].astype(BF16)
                bwd[layer, rows, :] = out[1][layer].astype(BF16)
    for layer in range(layers):
        for dst, axis in ((wd, 1), (wt, 0)):
            wide = lax.dot_general(wmix[layer], spread[...], (((axis,), (0,)), ((), ())), preferred_element_type=F32)
            full = jnp.concatenate([wide] * reps, axis=0)
            dst[layer] = jnp.where(same[...] != 0, full, 0.0).astype(BF16)


def band_weights(filter_taps, w_mix, ysub, nz):
    layers, _, num_taps = filter_taps.shape
    chans = w_mix.shape[1]
    r, n = grid2(TILE, TILE)
    spread = jnp.asarray(r[:chans] == n % chans, BF16)
    same = jnp.asarray(r // chans == n // chans, jnp.int32)
    indices = [x_index(num_taps, chans), y_index(num_taps), z_index(num_taps, ysub, nz)]
    vmem_spec = pl.BlockSpec(memory_space=pltpu.VMEM)
    shapes = [i.shape for i in indices for _ in range(2)] + [(TILE, TILE)] * 2
    return pl.pallas_call(
        band_kernel,
        out_shape=[jax.ShapeDtypeStruct((layers,) + shape, BF16) for shape in shapes],
        in_specs=[pl.BlockSpec(memory_space=pltpu.SMEM)] + [vmem_spec] * 6,
        out_specs=[vmem_spec] * 8,
        name='band_weights',
    )(filter_taps, w_mix, spread, same, *[jnp.asarray(i) for i in indices])


def entry_kernel(src, dst, rows):
    chans, nx, sub, nz = src.shape

    @pl.loop(0, nx)
    def _(x):
        part = src[:, x].astype(F32).reshape(chans * sub, nz)
        rows[pl.ds(pl.multiple_of(x * chans * sub, chans * sub), chans * sub), :] = part

    eye = (lax.broadcasted_iota(jnp.int32, (nz, nz), 0) == lax.broadcasted_iota(jnp.int32, (nz, nz), 1)).astype(BF16)

    @pl.loop(0, nx * chans // TILE)
    def _(tile):
        for y in range(sub):
            block = rows[pl.ds(tile * TILE * sub + y, TILE, stride=sub), :].astype(BF16)
            out = lax.dot_general(eye, block, (((1,), (1,)), ((), ())), preferred_element_type=F32)
            dst[y, :, lane_ds(tile)] = out.astype(BF16)


def to_dense(a):
    chans, nx, ny, nz = a.shape
    lanes = nx * chans
    return pl.pallas_call(
        entry_kernel,
        grid=(ny // SUB,),
        in_specs=[pl.BlockSpec((chans, nx, SUB, nz), lambda i: (0, 0, i, 0))],
        out_specs=pl.BlockSpec((SUB, nz, lanes), lambda i: (i, 0, 0)),
        out_shape=jax.ShapeDtypeStruct((ny, nz, lanes), BF16),
        scratch_shapes=[pltpu.VMEM((lanes * SUB, nz), F32)],
        compiler_params=pltpu.CompilerParams(vmem_limit_bytes=VMEM_BYTES),
        name='to_dense',
    )(a)


def leave_kernel(src, dst, rows):
    sub, nz, lanes = src.shape
    chans, nx = dst.shape[:2]
    eye = (lax.broadcasted_iota(jnp.int32, (TILE, TILE), 0) == lax.broadcasted_iota(jnp.int32, (TILE, TILE), 1)).astype(BF16)
    pad = jnp.zeros((LANE - nz, TILE), BF16)

    @pl.loop(0, lanes // TILE)
    def _(tile):
        for y in range(0, sub, 2):
            block = jnp.concatenate([src[y, :, lane_ds(tile)], pad, src[y + 1, :, lane_ds(tile)], pad], axis=0)
            out = lax.dot_general(eye, block, (((1,), (1,)), ((), ())), preferred_element_type=F32)
            rows[pl.ds(tile * TILE * sub + y, TILE, stride=sub), :] = out[:, :LANE]
            rows[pl.ds(tile * TILE * sub + y + 1, TILE, stride=sub), :] = out[:, LANE:]

    @pl.loop(0, nx)
    def _(x):
        part = rows[pl.ds(pl.multiple_of(x * chans * sub, chans * sub), chans * sub), :]
        dst[:, x] = part[:, :nz].astype(BF16).reshape(chans, sub, nz)


def from_dense(a, chans):
    ny, nz, lanes = a.shape
    nx = lanes // chans
    return pl.pallas_call(
        leave_kernel,
        grid=(ny // SUB,),
        in_specs=[pl.BlockSpec((SUB, nz, lanes), lambda i: (i, 0, 0))],
        out_specs=pl.BlockSpec((chans, nx, SUB, nz), lambda i: (0, 0, i, 0)),
        out_shape=jax.ShapeDtypeStruct((chans, nx, ny, nz), BF16),
        scratch_shapes=[pltpu.VMEM((lanes * SUB, LANE), F32)],
        compiler_params=pltpu.CompilerParams(vmem_limit_bytes=VMEM_BYTES),
        name='from_dense',
    )(a)


def dims(shape, half):
    ny, nz, lanes = shape
    group = ROWS - 2 * half
    return ny, nz, lanes, lanes // TILE, group, group // 2


def lane_ds(tile):
    return pl.ds(pl.multiple_of(tile * TILE, TILE), TILE)


class Links:
    def __init__(self, sizes):
        self.sizes = sizes
        self.pos = {name: lax.axis_index(name) for name in ('gx', 'gy', 'gz')}

    def barrier(self):
        sem = pltpu.get_barrier_semaphore()
        count = 1
        pl.semaphore_signal(sem, inc=1, device_id={'gx': 1 - self.pos['gx']}, device_id_type=MESH)
        for name in ('gy', 'gz'):
            size = self.sizes[name]
            for step in (1, size - 1):
                pl.semaphore_signal(sem, inc=1, device_id={name: lax.rem(self.pos[name] + step, size)}, device_id_type=MESH)
                count += 1
        pl.semaphore_wait(sem, count)

    def pair(self, name, low_src, high_dst, high_src, low_dst, sems, tile):
        send, recv = sems
        pos, size = self.pos[name], self.sizes[name]
        down = pltpu.make_async_remote_copy(low_src, high_dst, send.at[0, tile], recv.at[0, tile], device_id={name: jnp.maximum(pos - 1, 0)}, device_id_type=MESH)
        up = pltpu.make_async_remote_copy(high_src, low_dst, send.at[1, tile], recv.at[1, tile], device_id={name: jnp.minimum(pos + 1, size - 1)}, device_id_type=MESH)
        return (down, pos > 0), (up, pos < size - 1)

    def start(self, flows):
        for copy, has in flows:
            pl.when(has)(copy.start)

    def wait_recv(self, flows):
        (down, has_low), (up, has_high) = flows
        pl.when(has_high)(down.wait_recv)
        pl.when(has_low)(up.wait_recv)

    def wait_send(self, flows):
        for copy, has in flows:
            pl.when(has)(copy.wait_send)

    def zero_edges(self, name, low_ref, high_ref):
        @pl.when(self.pos[name] == 0)
        def _():
            low_ref[...] = jnp.zeros_like(low_ref)

        @pl.when(self.pos[name] == self.sizes[name] - 1)
        def _():
            high_ref[...] = jnp.zeros_like(high_ref)

    def x_edge(self, ext, sems, lanes):
        send, recv = sems
        me = self.pos['gx']
        src = pl.multiple_of(lanes + me * (TILE - lanes), TILE)
        dst = pl.multiple_of(me * (lanes + TILE), TILE)
        return pltpu.make_async_remote_copy(ext.at[:, :, pl.ds(src, TILE)], ext.at[:, :, pl.ds(dst, TILE)], send, recv, device_id={'gx': 1 - me}, device_id_type=MESH)

    def zero_x(self, ext, lanes):
        start = pl.multiple_of((1 - self.pos['gx']) * 0 + self.pos['gx'] * (lanes + TILE), TILE)
        ny = ext.shape[0]

        @pl.loop(0, ny)
        def _(y):
            ext[y, :, pl.ds(start, TILE)] = jnp.zeros((ext.shape[1], TILE), ext.dtype)


def y_flows(links, buf, half, ny, sems, tile):
    cols = lane_ds(tile)
    return links.pair('gy', buf.at[pl.ds(half, half), :, cols], buf.at[pl.ds(ny + half, half), :, cols], buf.at[pl.ds(ny, half), :, cols], buf.at[pl.ds(0, half), :, cols], sems, tile)


def z_flows(links, zs, zr, sems, tile):
    cols = lane_ds(tile)
    return links.pair('gz', zs.at[0, :, :, cols], zr.at[1, :, :, cols], zs.at[1, :, :, cols], zr.at[0, :, :, cols], sems, tile)


def dot(a, b):
    return jnp.dot(a, b, preferred_element_type=F32)


def x_pass_rows(ext, wx, tile, start, count):
    nz = ext.shape[1]
    block = ext[pl.ds(start, count), :, pl.ds(pl.multiple_of(tile * TILE, TILE), 3 * TILE)]
    return dot(block.reshape(count * nz, 3 * TILE), wx[...])


def fwd_kernel(half, sizes, last, *refs):
    if last:
        (v_hbm, wx, ly, lz, wd, bias, a3_hbm, vext, a1, a2, a3, zs, zr, in_sem, out_sem, xsend, xrecv, ysend, yrecv, zsend, zrecv) = refs
    else:
        (v_hbm, wx, ly, lz, wd, bias, a3_hbm, vo_hbm, vext, a1, a2, a3, zs, zr, in_sem, out_sem, xsend, xrecv, ysend, yrecv, zsend, zrecv) = refs
    ny, nz, lanes, tiles, group, ysub = dims(v_hbm.shape, half)
    links = Links(sizes)
    me = links.pos['gx']

    def order(step):
        return step + me * (tiles - 1 - 2 * step)

    def fetch(tile):
        return pltpu.make_async_copy(v_hbm.at[:, :, lane_ds(tile)], vext.at[:, :, lane_ds(tile + 1)], in_sem.at[tile])

    edge = order(tiles - 1)
    fetch(edge).start()
    for step in range(tiles - 1):
        fetch(order(step)).start()
    links.zero_edges('gy', a1.at[pl.ds(0, half)], a1.at[pl.ds(ny + half, half)])
    links.zero_edges('gz', zr.at[0], zr.at[1])
    links.zero_x(vext, lanes)
    links.barrier()
    fetch(edge).wait()
    xcopy = links.x_edge(vext, (xsend, xrecv), lanes)
    xcopy.start()
    fetch(order(0)).wait()

    def x_phase(tile):
        count = 8 if ny % 8 == 0 else ysub
        for y in range(0, ny, count):
            out = x_pass_rows(vext, wx, tile, y, count)
            a1[pl.ds(y + half, count), :, lane_ds(tile)] = out.astype(BF16).reshape(count, nz, TILE)
        links.start(y_flows(links, a1, half, ny, (ysend, yrecv), tile))

    @pl.loop(0, tiles - 1)
    def _(step):
        @pl.when(step < tiles - 2)
        def _():
            fetch(order(step + 1)).wait()
        x_phase(order(step))

    xcopy.wait_recv()
    x_phase(edge)

    @pl.loop(0, tiles)
    def _(step):
        tile = order(step)
        cols = lane_ds(tile)
        links.wait_recv(y_flows(links, a1, half, ny, (ysend, yrecv), tile))
        for g in range(ny // group):
            for zb in range(nz // ROWS):
                side = {0: 0, nz // ROWS - 1: 1}.get(zb)
                rhs = a1[pl.ds(g * group, ROWS), pl.ds(zb * ROWS, ROWS), cols].reshape(ROWS * ROWS, TILE)
                main = group * ROWS
                if side == 0:
                    lhs = ly[pl.ds(0, main + 2 * ROWS), :]
                elif side == 1:
                    lhs = jnp.concatenate([ly[pl.ds(0, main), :], ly[pl.ds(main + 2 * ROWS, 2 * ROWS), :]], axis=0)
                else:
                    lhs = ly[pl.ds(0, main), :]
                out = dot(lhs, rhs).astype(BF16)
                a2[pl.ds(g * group, group), pl.ds(zb * ROWS, ROWS), cols] = out[: group * ROWS].reshape(group, ROWS, TILE)
                if side is not None:
                    zs[side, pl.ds(2 * g, 2), :, cols] = out[group * ROWS :].reshape(2, ROWS, TILE)
        links.start(z_flows(links, zs, zr, (zsend, zrecv), tile))

    xcopy.wait_send()

    def put_a3(tile):
        return pltpu.make_async_copy(a3.at[:, :, lane_ds(tile)], a3_hbm.at[:, :, lane_ds(tile)], out_sem.at[0, tile])

    def put_v(tile):
        return pltpu.make_async_copy(vext.at[:, :, lane_ds(tile + 1)], vo_hbm.at[:, :, lane_ds(tile)], out_sem.at[1, tile])

    @pl.loop(0, tiles)
    def _(step):
        tile = order(step)
        cols = lane_ds(tile)
        links.wait_recv(z_flows(links, zs, zr, (zsend, zrecv), tile))
        for g in range(ny // ysub):
            main = a2[pl.ds(g * ysub, ysub), :, cols].reshape(ysub * nz, TILE)
            rhs = jnp.concatenate([main, zr[0, g, :, cols], zr[1, g, :, cols]], axis=0)
            out = dot(lz[...], rhs).astype(BF16)
            a3[pl.ds(g * ysub, ysub), :, cols] = out.reshape(ysub, nz, TILE)
            if not last:
                pre = dot(out, wd[...]) + bias[...]
                act = 0.5 * pre * (1.0 + lax.erf(pre * INV_SQRT2))
                vcols = lane_ds(tile + 1)
                old = vext[pl.ds(g * ysub, ysub), :, vcols].astype(F32).reshape(ysub * nz, TILE)
                vext[pl.ds(g * ysub, ysub), :, vcols] = (old + act).astype(BF16).reshape(ysub, nz, TILE)
        put_a3(tile).start()
        if not last:
            put_v(tile).start()

    @pl.loop(0, tiles)
    def _(tile):
        links.wait_send(y_flows(links, a1, half, ny, (ysend, yrecv), tile))
        links.wait_send(z_flows(links, zs, zr, (zsend, zrecv), tile))
        put_a3(tile).wait()
        if not last:
            put_v(tile).wait()


def bwd_kernel(half, sizes, a3_hbm, g_hbm, wx, ly, lz, pick, wd, wt, bias, go_hbm, dw_ref, db_ref, a3, grad, sb, d3, d2, dext, zs, zr, in_sem, out_sem, xsend, xrecv, ysend, yrecv, zsend, zrecv):
    ny, nz, lanes, tiles, group, ysub = dims(g_hbm.shape, half)
    links = Links(sizes)
    me = links.pos['gx']

    def order(step):
        return (tiles - 1 - step) + me * (2 * step - tiles + 1)

    def fetch(tile):
        cols = lane_ds(tile)
        return (pltpu.make_async_copy(a3_hbm.at[:, :, cols], a3.at[:, :, cols], in_sem.at[0, tile]), pltpu.make_async_copy(g_hbm.at[:, :, cols], grad.at[:, :, cols], in_sem.at[1, tile]))

    for step in range(tiles):
        for copy in fetch(order(step)):
            copy.start()
    links.zero_edges('gy', d2.at[pl.ds(0, half)], d2.at[pl.ds(ny + half, half)])
    links.zero_edges('gz', zr.at[0], zr.at[1])
    links.zero_x(dext, lanes)
    dw_ref[...] = jnp.zeros_like(dw_ref)
    db_ref[...] = jnp.zeros_like(db_ref)
    links.barrier()

    @pl.loop(0, tiles)
    def _(step):
        tile = order(step)
        cols = lane_ds(tile)
        for copy in fetch(tile):
            copy.wait()
        for g in range(ny // ysub):
            rows = pl.ds(g * ysub, ysub)
            act = a3[rows, :, cols].reshape(ysub * nz, TILE)
            pre = dot(act, wd[...]) + bias[...]
            cot = grad[rows, :, cols].astype(F32).reshape(ysub * nz, TILE)
            slope = 0.5 + 0.5 * lax.erf(pre * INV_SQRT2) + pre * (INV_SQRT_2PI * jnp.exp(-0.5 * pre * pre))
            scaled = slope * cot
            db_ref[...] += jnp.sum(scaled.reshape(ysub * nz // 8, 8, TILE), axis=0)
            low = scaled.astype(BF16)
            sb[pl.ds(g * ysub * nz, ysub * nz), :] = low
            mixed = dot(low, wt[...]).astype(BF16)
            d3[rows, :, cols] = mixed.reshape(ysub, nz, TILE)
            planes = dot(pick[...], mixed).astype(BF16)
            zs[0, g, :, cols] = planes[:ROWS]
            zs[1, g, :, cols] = planes[ROWS:]
        links.start(z_flows(links, zs, zr, (zsend, zrecv), tile))
        acts = a3[:, :, cols].reshape(ny * nz, TILE)
        dw_ref[...] += lax.dot_general(acts, sb[...], (((0,), (0,)), ((), ())), preferred_element_type=F32)

    @pl.loop(0, tiles)
    def _(step):
        tile = order(step)
        cols = lane_ds(tile)
        links.wait_recv(z_flows(links, zs, zr, (zsend, zrecv), tile))
        for g in range(ny // ysub):
            main = d3[pl.ds(g * ysub, ysub), :, cols].reshape(ysub * nz, TILE)
            rhs = jnp.concatenate([main, zr[0, g, :, cols], zr[1, g, :, cols]], axis=0)
            out = dot(lz[...], rhs).astype(BF16)
            d2[pl.ds(g * ysub + half, ysub), :, cols] = out.reshape(ysub, nz, TILE)
        links.start(y_flows(links, d2, half, ny, (ysend, yrecv), tile))

    xcopy = links.x_edge(dext, (xsend, xrecv), lanes)

    @pl.loop(0, tiles)
    def _(step):
        tile = order(step)
        cols = lane_ds(tile)
        links.wait_recv(y_flows(links, d2, half, ny, (ysend, yrecv), tile))
        for g in range(ny // group):
            for zb in range(nz // ROWS):
                rhs = d2[pl.ds(g * group, ROWS), pl.ds(zb * ROWS, ROWS), cols].reshape(ROWS * ROWS, TILE)
                out = dot(ly[pl.ds(0, group * ROWS), :], rhs).astype(BF16)
                dext[pl.ds(g * group, group), pl.ds(zb * ROWS, ROWS), lane_ds(tile + 1)] = out.reshape(group, ROWS, TILE)
        pl.when(step == 0)(xcopy.start)

    def put(tile):
        return pltpu.make_async_copy(grad.at[:, :, lane_ds(tile)], go_hbm.at[:, :, lane_ds(tile)], out_sem.at[tile])

    def x_phase(tile):
        cols = lane_ds(tile)
        count = 8 if ny % 8 == 0 else ysub
        for y in range(0, ny, count):
            rows = pl.ds(y, count)
            spread = x_pass_rows(dext, wx, tile, y, count)
            old = grad[rows, :, cols].astype(F32).reshape(count * nz, TILE)
            grad[rows, :, cols] = (old + spread).astype(BF16).reshape(count, nz, TILE)
        put(tile).start()

    @pl.loop(0, tiles - 1)
    def _(step):
        x_phase(order(tiles - 1 - step))

    xcopy.wait_recv()
    x_phase(order(0))
    xcopy.wait_send()

    @pl.loop(0, tiles)
    def _(tile):
        links.wait_send(y_flows(links, d2, half, ny, (ysend, yrecv), tile))
        links.wait_send(z_flows(links, zs, zr, (zsend, zrecv), tile))
        put(tile).wait()


def link_sems(tiles):
    dma = pltpu.SemaphoreType.DMA
    return [dma, dma, dma((2, tiles)), dma((2, tiles)), dma((2, tiles)), dma((2, tiles))]


def solution(mesh):
    names = ('gx', 'gy', 'gz')
    sizes = {name: mesh.shape[name] for name in names}
    vol_spec = P('dp', 'gx', 'gy', 'gz')
    any_spec = pl.BlockSpec(memory_space=pl.ANY)
    vmem_spec = pl.BlockSpec(memory_space=pltpu.VMEM)
    dma = pltpu.SemaphoreType.DMA

    def local_step(volume, cot_out, filter_taps, w_mix, b_mix):
        chans, nx, ny, nz = volume.shape
        num_layers, _, num_taps = filter_taps.shape
        half = (num_taps - 1) // 2
        lanes = nx * chans
        tiles = lanes // TILE
        reps = TILE // chans
        group = ROWS - 2 * half
        ysub = group // 2
        params = functools.partial(pltpu.CompilerParams, has_side_effects=True, vmem_limit_bytes=VMEM_BYTES)
        block = jax.ShapeDtypeStruct((ny, nz, lanes), BF16)
        wx_f, wx_b, ly_f, ly_b, lz_f, lz_b, wd, wt = band_weights(filter_taps, w_mix, ysub, nz)
        pick = pick_matrix(half, ysub, nz)
        bias = jnp.tile(b_mix, (1, reps))[:, None, :]

        halo = pltpu.VMEM((2, ny // ysub, ROWS, lanes), BF16)
        full = pltpu.VMEM((ny, nz, lanes), BF16)
        tall = pltpu.VMEM((ny + 2 * half, nz, lanes), BF16)
        wide = pltpu.VMEM((ny, nz, lanes + 2 * TILE), BF16)

        cur = to_dense(volume)
        acts = []
        for layer in range(num_layers):
            last = layer + 1 == num_layers
            outs = pl.pallas_call(
                functools.partial(fwd_kernel, half, sizes, last),
                out_shape=[block] * (1 if last else 2),
                in_specs=[any_spec] + [vmem_spec] * 5,
                out_specs=[any_spec] * (1 if last else 2),
                scratch_shapes=[wide, tall, full, full, halo, halo, dma((tiles,)), dma((2, tiles))] + link_sems(tiles),
                compiler_params=params(collective_id=layer),
                name='fwd_layer',
            )(cur, wx_f[layer], ly_f[layer], lz_f[layer], wd[layer], bias[layer])
            acts.append(outs[0])
            if not last:
                cur = outs[1]

        grad = to_dense(cot_out)
        grad_w, grad_b = [None] * num_layers, [None] * num_layers
        for layer in reversed(range(num_layers)):
            grad, dw, db = pl.pallas_call(
                functools.partial(bwd_kernel, half, sizes),
                out_shape=[block, jax.ShapeDtypeStruct((TILE, TILE), F32), jax.ShapeDtypeStruct((8, TILE), F32)],
                in_specs=[any_spec] * 2 + [vmem_spec] * 7,
                out_specs=[any_spec, vmem_spec, vmem_spec],
                scratch_shapes=[full, full, pltpu.VMEM((ny * nz, TILE), BF16), full, tall, wide, halo, halo, dma((2, tiles)), dma((tiles,))] + link_sems(tiles),
                compiler_params=params(collective_id=num_layers + layer),
                name='bwd_layer',
            )(acts[layer], grad, wx_b[layer], ly_b[layer], lz_b[layer], pick, wd[layer], wt[layer], bias[layer])
            dw4 = dw.reshape(reps, chans, reps, chans)
            grad_w[layer] = sum(dw4[i, :, i, :] for i in range(reps))
            grad_b[layer] = jnp.sum(db.reshape(8 * reps, chans), axis=0)
        grad_volume = from_dense(grad, chans)
        grad_w_sum = lax.psum(jnp.stack(grad_w), names)
        grad_b_sum = lax.psum(jnp.stack(grad_b), names)
        return grad_volume, grad_w_sum, grad_b_sum

    return jax.shard_map(local_step, mesh=mesh, in_specs=(vol_spec, vol_spec, P(), P(), P()), out_specs=(vol_spec, P('dp'), P('dp')), check_vma=False)
```

```python
import functools

import jax
import jax.numpy as jnp
import numpy as np
from jax import lax
from jax.experimental import pallas as pl
from jax.experimental.pallas import tpu as pltpu
from jax.sharding import PartitionSpec as P

MESH = pl.DeviceIdType.MESH
TILE = 256
ROWS = 16
LANE = 128
SUB = 8
VMEM_BYTES = 60 * 1024 * 1024
INV_SQRT2 = 0.7071067811865476
TWO_INV_SQRT_PI = 1.1283791670955126
F32 = jnp.float32
BF16 = jnp.bfloat16


def valid_index(index, keep, num_taps):
    return np.where(keep & (index >= 0) & (index < num_taps), index, -1).astype(np.int32)


def grid2(rows, cols):
    return np.arange(rows)[:, None], np.arange(cols)[None, :]


def x_index(num_taps, chans):
    r, n = grid2(3 * TILE, TILE)
    index = r // chans - TILE // chans - n // chans + num_taps // 2
    return valid_index(index, r % chans == n % chans, num_taps)


def y_index(num_taps):
    half = num_taps // 2
    group = ROWS - 2 * half
    r, k = grid2(group * ROWS, ROWS * ROWS)
    yi, zi = k // ROWS, k % ROWS
    parts = [valid_index(yi - r // ROWS, r % ROWS == zi, num_taps)]
    r, k = grid2(2 * ROWS, ROWS * ROWS)
    q = r % ROWS
    yo = r // ROWS * (group // 2) + q // half
    for first in (0, ROWS - half):
        keep = (q % half + first == zi) & (q < (group // 2) * half)
        parts.append(valid_index(yi - yo, keep, num_taps))
    return np.concatenate(parts, axis=0)


def z_index(num_taps, ysub, nz):
    half = num_taps // 2
    r, k = grid2(ysub * nz, ysub * nz + 2 * ROWS)
    yo, zo = r // nz, r % nz
    is_main = k < ysub * nz
    q = (k - ysub * nz) % ROWS
    low = k < ysub * nz + ROWS
    yi = np.where(is_main, k // nz, q // half)
    zi = np.where(is_main, k % nz, np.where(low, q % half - half, nz + q % half))
    keep = (yi == yo) & (is_main | (q < ysub * half))
    return valid_index(zi - zo + half, keep, num_taps)


def pick_matrix(half, ysub, nz):
    r, k = grid2(2 * ROWS, ysub * nz)
    q = r % ROWS
    zo = q % half + np.where(r < ROWS, 0, nz - half)
    hit = (k // nz == q // half) & (k % nz == zo) & (q < ysub * half)
    return jnp.asarray(hit, BF16)


def band_kernel(taps, wmix, spread, same, xi, yi, zi, xf, xb, yf, yb, zf, zb, wd, wt):
    layers, _, num_taps = taps.shape
    reps = TILE // spread.shape[0]
    for axis, index, fwd, bwd in ((0, xi, xf, xb), (1, yi, yf, yb), (2, zi, zf, zb)):
        @pl.loop(0, index.shape[0] // ROWS)
        def _(chunk):
            rows = pl.ds(pl.multiple_of(chunk * ROWS, ROWS), ROWS)
            which = index[rows, :]
            zero = jnp.zeros(which.shape, F32)
            out = [[zero] * layers, [zero] * layers]
            for t in range(num_taps):
                hit = which == t
                for layer in range(layers):
                    out[0][layer] = jnp.where(hit, taps[layer, axis, t], out[0][layer])
                    out[1][layer] = jnp.where(hit, taps[layer, axis, num_taps - 1 - t], out[1][layer])
            for layer in range(layers):
                fwd[layer, rows, :] = out[0][layer].astype(BF16)
                bwd[layer, rows, :] = out[1][layer].astype(BF16)
    for layer in range(layers):
        for dst, axis in ((wd, 1), (wt, 0)):
            wide = lax.dot_general(wmix[layer], spread[...], (((axis,), (0,)), ((), ())), preferred_element_type=F32)
            full = jnp.concatenate([wide] * reps, axis=0)
            dst[layer] = jnp.where(same[...] != 0, full, 0.0).astype(BF16)


def band_weights(filter_taps, w_mix, ysub, nz):
    layers, _, num_taps = filter_taps.shape
    chans = w_mix.shape[1]
    r, n = grid2(TILE, TILE)
    spread = jnp.asarray(r[:chans] == n % chans, BF16)
    same = jnp.asarray(r // chans == n // chans, jnp.int32)
    indices = [x_index(num_taps, chans), y_index(num_taps), z_index(num_taps, ysub, nz)]
    vmem_spec = pl.BlockSpec(memory_space=pltpu.VMEM)
    shapes = [i.shape for i in indices for _ in range(2)] + [(TILE, TILE)] * 2
    return pl.pallas_call(
        band_kernel,
        out_shape=[jax.ShapeDtypeStruct((layers,) + shape, BF16) for shape in shapes],
        in_specs=[pl.BlockSpec(memory_space=pltpu.SMEM)] + [vmem_spec] * 6,
        out_specs=[vmem_spec] * 8,
        name='band_weights',
    )(filter_taps, w_mix, spread, same, *[jnp.asarray(i) for i in indices])


def entry_kernel(src, dst, rows):
    chans, nx, sub, nz = src.shape

    @pl.loop(0, nx)
    def _(x):
        part = src[:, x].astype(F32).reshape(chans * sub, nz)
        rows[pl.ds(pl.multiple_of(x * chans * sub, chans * sub), chans * sub), :] = part

    eye = (lax.broadcasted_iota(jnp.int32, (nz, nz), 0) == lax.broadcasted_iota(jnp.int32, (nz, nz), 1)).astype(BF16)

    @pl.loop(0, nx * chans // TILE)
    def _(tile):
        for y in range(sub):
            block = rows[pl.ds(tile * TILE * sub + y, TILE, stride=sub), :].astype(BF16)
            out = lax.dot_general(eye, block, (((1,), (1,)), ((), ())), preferred_element_type=F32)
            dst[y, :, lane_ds(tile)] = out.astype(BF16)


def to_dense(a):
    chans, nx, ny, nz = a.shape
    lanes = nx * chans
    return pl.pallas_call(
        entry_kernel,
        grid=(ny // SUB,),
        in_specs=[pl.BlockSpec((chans, nx, SUB, nz), lambda i: (0, 0, i, 0))],
        out_specs=pl.BlockSpec((SUB, nz, lanes), lambda i: (i, 0, 0)),
        out_shape=jax.ShapeDtypeStruct((ny, nz, lanes), BF16),
        scratch_shapes=[pltpu.VMEM((lanes * SUB, nz), F32)],
        compiler_params=pltpu.CompilerParams(vmem_limit_bytes=VMEM_BYTES),
        name='to_dense',
    )(a)


def leave_kernel(src, dst, rows):
    sub, nz, lanes = src.shape
    chans, nx = dst.shape[:2]
    eye = (lax.broadcasted_iota(jnp.int32, (TILE, TILE), 0) == lax.broadcasted_iota(jnp.int32, (TILE, TILE), 1)).astype(BF16)
    pad = jnp.zeros((LANE - nz, TILE), BF16)

    @pl.loop(0, lanes // TILE)
    def _(tile):
        for y in range(0, sub, 2):
            block = jnp.concatenate([src[y, :, lane_ds(tile)], pad, src[y + 1, :, lane_ds(tile)], pad], axis=0)
            out = lax.dot_general(eye, block, (((1,), (1,)), ((), ())), preferred_element_type=F32)
            rows[pl.ds(tile * TILE * sub + y, TILE, stride=sub), :] = out[:, :LANE]
            rows[pl.ds(tile * TILE * sub + y + 1, TILE, stride=sub), :] = out[:, LANE:]

    @pl.loop(0, nx)
    def _(x):
        part = rows[pl.ds(pl.multiple_of(x * chans * sub, chans * sub), chans * sub), :]
        dst[:, x] = part[:, :nz].astype(BF16).reshape(chans, sub, nz)


def from_dense(a, chans):
    ny, nz, lanes = a.shape
    nx = lanes // chans
    return pl.pallas_call(
        leave_kernel,
        grid=(ny // SUB,),
        in_specs=[pl.BlockSpec((SUB, nz, lanes), lambda i: (i, 0, 0))],
        out_specs=pl.BlockSpec((chans, nx, SUB, nz), lambda i: (0, 0, i, 0)),
        out_shape=jax.ShapeDtypeStruct((chans, nx, ny, nz), BF16),
        scratch_shapes=[pltpu.VMEM((lanes * SUB, LANE), F32)],
        compiler_params=pltpu.CompilerParams(vmem_limit_bytes=VMEM_BYTES),
        name='from_dense',
    )(a)


def dims(shape, half):
    ny, nz, lanes = shape
    group = ROWS - 2 * half
    return ny, nz, lanes, lanes // TILE, group, group // 2


def lane_ds(tile):
    return pl.ds(pl.multiple_of(tile * TILE, TILE), TILE)


class Links:
    def __init__(self, sizes):
        self.sizes = sizes
        self.pos = {name: lax.axis_index(name) for name in ('gx', 'gy', 'gz')}

    def barrier(self):
        sem = pltpu.get_barrier_semaphore()
        count = 0
        for name, size in self.sizes.items():
            for step in range(1, size):
                pl.semaphore_signal(sem, inc=1, device_id={name: lax.rem(self.pos[name] + step, size)}, device_id_type=MESH)
                count += 1
        pl.semaphore_wait(sem, count)

    def pair(self, name, low_src, high_src, dst, sems, slot, tile):
        send, recv = sems
        pos, size = self.pos[name], self.sizes[name]
        down = pltpu.make_async_remote_copy(low_src, dst[1], send.at[0, tile], recv.at[slot, 0, tile], device_id={name: jnp.maximum(pos - 1, 0)}, device_id_type=MESH)
        up = pltpu.make_async_remote_copy(high_src, dst[0], send.at[1, tile], recv.at[slot, 1, tile], device_id={name: jnp.minimum(pos + 1, size - 1)}, device_id_type=MESH)
        return (down, pos > 0), (up, pos < size - 1)

    def start(self, flows):
        for copy, has in flows:
            pl.when(has)(copy.start)

    def wait_recv(self, flows):
        (down, has_low), (up, has_high) = flows
        pl.when(has_high)(down.wait_recv)
        pl.when(has_low)(up.wait_recv)

    def wait_send(self, flows):
        for copy, has in flows:
            pl.when(has)(copy.wait_send)

    def zero_edges(self, name, halos):
        for side, at in ((0, 0), (1, self.sizes[name] - 1)):
            @pl.when(self.pos[name] == at)
            def _():
                for slot in range(2):
                    halos[slot, side] = jnp.zeros(halos.shape[2:], halos.dtype)

    def x_edge(self, src, xh, sems, slot, lanes):
        send, recv = sems
        me = self.pos['gx']
        first = pl.multiple_of((1 - me) * (lanes - TILE), TILE)
        return pltpu.make_async_remote_copy(src.at[:, :, pl.ds(first, TILE)], xh.at[slot], send, recv.at[slot], device_id={'gx': 1 - me}, device_id_type=MESH)


def y_flows(links, buf, halos, sems, slot, tile):
    cols = lane_ds(tile)
    ny, half = buf.shape[0], halos.shape[2]
    dst = [halos.at[slot, side, :, :, cols] for side in range(2)]
    return links.pair('gy', buf.at[pl.ds(0, half), :, cols], buf.at[pl.ds(ny - half, half), :, cols], dst, sems, slot, tile)


def z_flows(links, zs, zr, sems, slot, tile):
    cols = lane_ds(tile)
    dst = [zr.at[slot, side, :, :, cols] for side in range(2)]
    return links.pair('gz', zs.at[0, :, :, cols], zs.at[1, :, :, cols], dst, sems, slot, tile)


def dot(a, b):
    return jnp.dot(a, b, preferred_element_type=F32)


def x_stage(src, xh, wx, me, layer, slot, tile, outer, edge, before_edge, emit):
    ny, nz, lanes = src.shape
    count = 8
    far, near = lanes - 2 * TILE, 0

    def rows(y, lane, width, weight):
        block = src[pl.ds(y, count), :, pl.ds(pl.multiple_of(lane, TILE), width)]
        return dot(block.reshape(count * nz, width), weight)

    @pl.when(outer)
    def _():
        weight = wx[layer, pl.ds(pl.multiple_of((1 - me) * TILE, TILE), 2 * TILE), :]
        for y in range(0, ny, count):
            emit(y, count, rows(y, me * far, 2 * TILE, weight))

    @pl.when(jnp.logical_not(outer | edge))
    def _():
        weight = wx[layer]
        for y in range(0, ny, count):
            emit(y, count, rows(y, (tile - 1) * TILE, 3 * TILE, weight))

    @pl.when(edge)
    def _():
        before_edge()
        weight = wx[layer, pl.ds(pl.multiple_of(me * TILE, TILE), 2 * TILE), :]
        other = wx[layer, pl.ds(pl.multiple_of((1 - me) * 2 * TILE, TILE), TILE), :]
        for y in range(0, ny, count):
            outside = dot(xh[slot, pl.ds(y, count)].reshape(count * nz, TILE), other)
            emit(y, count, rows(y, (1 - me) * far, 2 * TILE, weight) + outside)


def y_stage(src, halos, ly, layer, slot, tile, picks, emit):
    ny, nz, lanes, tiles, group, ysub = dims(src.shape, halos.shape[2])
    half = halos.shape[2]
    cols = lane_ds(tile)
    main = group * ROWS
    base = ly[layer, pl.ds(0, main), :]
    low = ly[layer, pl.ds(0, main + 2 * ROWS), :]
    high = jnp.concatenate([base, ly[layer, pl.ds(main + 2 * ROWS, 2 * ROWS), :]], axis=0)
    for g in range(ny // group):
        for zb in range(nz // ROWS):
            zrows = pl.ds(zb * ROWS, ROWS)
            first, last = g * group - half, g * group - half + ROWS
            parts = []
            if first < 0:
                parts.append(halos[slot, 0, :, zrows, cols])
            parts.append(src[pl.ds(max(first, 0), min(last, ny) - max(first, 0)), zrows, cols])
            if last > ny:
                parts.append(halos[slot, 1, :, zrows, cols])
            rhs = jnp.concatenate(parts, axis=0) if len(parts) > 1 else parts[0]
            side = {0: 0, nz // ROWS - 1: 1}.get(zb) if picks else None
            lhs = {None: base, 0: low, 1: high}[side]
            emit(g, zb, side, dot(lhs, rhs.reshape(ROWS * ROWS, TILE)).astype(BF16))


def z_stage(src, zr, lz, layer, slot, tile, ysub, emit):
    ny, nz, lanes = src.shape
    cols = lane_ds(tile)
    lhs = lz[layer]
    for g in range(ny // ysub):
        main = src[pl.ds(g * ysub, ysub), :, cols].reshape(ysub * nz, TILE)
        rhs = jnp.concatenate([main, zr[slot, 0, g, :, cols], zr[slot, 1, g, :, cols]], axis=0)
        emit(g, dot(lhs, rhs).astype(BF16).reshape(ysub, nz, TILE))


def fwd_kernel(half, sizes, v_hbm, wx, ly, lz, wd, bias, a3_hbm, vol, xh, a1, yr, a2, zs, zr, a3, in_sem, out_sem, xsend, xrecv, ysend, yrecv, zsend, zrecv):
    ny, nz, lanes, tiles, group, ysub = dims(v_hbm.shape, half)
    layers = wx.shape[0]
    links = Links(sizes)
    me = links.pos['gx']
    ysems, zsems, xsems = (ysend, yrecv), (zsend, zrecv), (xsend, xrecv)
    total = layers * tiles
    lag_y, lag_z = 2, 4
    assert lag_z <= tiles - 2

    def place(item):
        layer, p = item // tiles, lax.rem(item, tiles)
        return layer, p, p + me * (tiles - 1 - 2 * p), lax.rem(layer, 2)

    def fetch(tile):
        return pltpu.make_async_copy(v_hbm.at[:, :, lane_ds(tile)], vol.at[:, :, lane_ds(tile)], in_sem.at[tile])

    def put(layer, tile):
        return pltpu.make_async_copy(a3.at[:, :, lane_ds(tile)], a3_hbm.at[layer, :, :, lane_ds(tile)], out_sem.at[tile])

    def y_at(slot, tile):
        return y_flows(links, a1, yr, ysems, slot, tile)

    def z_at(slot, tile):
        return z_flows(links, zs, zr, zsems, slot, tile)

    def x_at(slot):
        return links.x_edge(vol, xh, xsems, slot, lanes)

    edge_tile = place(tiles - 1)[2]
    fetch(edge_tile).start()
    for p in range(tiles - 1):
        fetch(place(p)[2]).start()
    links.zero_edges('gy', yr)
    links.zero_edges('gz', zr)
    links.barrier()
    fetch(edge_tile).wait()
    x_at(0).start()

    @pl.loop(0, total + lag_z)
    def _(step):
        @pl.when(step < total)
        def _():
            layer, p, tile, slot = place(step)

            @pl.when(layer == 0)
            def _():
                pl.when(p == 0)(fetch(tile).wait)
                pl.when(p < tiles - 2)(fetch(place(p + 1)[2]).wait)

            @pl.when(layer > 0)
            def _():
                links.wait_send(y_at(1 - slot, tile))

            def before_edge():
                x_at(slot).wait_recv()
                x_at(slot).wait_send()

            def emit(y, count, out):
                a1[pl.ds(y, count), :, lane_ds(tile)] = out.astype(BF16).reshape(count, nz, TILE)

            x_stage(vol, xh, wx, me, layer, slot, tile, p == 0, p == tiles - 1, before_edge, emit)
            links.start(y_at(slot, tile))

        @pl.when((step >= lag_y) & (step < total + lag_y))
        def _():
            layer, p, tile, slot = place(step - lag_y)
            cols = lane_ds(tile)

            @pl.when(layer > 0)
            def _():
                links.wait_send(z_at(1 - slot, tile))

            links.wait_recv(y_at(slot, tile))

            def emit(g, zb, side, out):
                a2[pl.ds(g * group, group), pl.ds(zb * ROWS, ROWS), cols] = out[: group * ROWS].reshape(group, ROWS, TILE)
                if side is not None:
                    zs[side, pl.ds(2 * g, 2), :, cols] = out[group * ROWS :].reshape(2, ROWS, TILE)

            y_stage(a1, yr, ly, layer, slot, tile, True, emit)
            links.start(z_at(slot, tile))

        @pl.when(step >= lag_z)
        def _():
            layer, p, tile, slot = place(step - lag_z)
            cols = lane_ds(tile)

            @pl.when(layer > 0)
            def _():
                put(layer - 1, tile).wait()

            links.wait_recv(z_at(slot, tile))

            def emit(g, out):
                a3[pl.ds(g * ysub, ysub), :, cols] = out

            z_stage(a2, zr, lz, layer, slot, tile, ysub, emit)
            put(layer, tile).start()

            @pl.when(layer < layers - 1)
            def _():
                for g in range(ny // group):
                    rows = pl.ds(g * group, group)
                    pre = dot(a3[rows, :, cols].reshape(group * nz, TILE), wd[layer]) + bias[layer]
                    old = vol[rows, :, cols].astype(F32).reshape(group * nz, TILE)
                    new = old + (0.5 * pre) * (1.0 + lax.erf(pre * INV_SQRT2))
                    vol[rows, :, cols] = new.astype(BF16).reshape(group, nz, TILE)
                pl.when(p == tiles - 1)(x_at(1 - slot).start)

    @pl.loop(0, tiles)
    def _(tile):
        slot = (layers - 1) % 2
        links.wait_send(y_at(slot, tile))
        links.wait_send(z_at(slot, tile))
        put(layers - 1, tile).wait()


def bwd_kernel(half, sizes, chans, a3_hbm, g_hbm, wx, ly, lz, pick, wd, wt, bias, go_hbm, sums, acts, grad, sb, d3, zs, zr, d2, yr, d1, xh, dw, db, gathered, act_sem, in_sem, out_sem, gsend, grecv, xsend, xrecv, ysend, yrecv, zsend, zrecv):
    ny, nz, lanes, tiles, group, ysub = dims(g_hbm.shape, half)
    layers = wx.shape[0]
    links = Links(sizes)
    me = links.pos['gx']
    ysems, zsems, xsems = (ysend, yrecv), (zsend, zrecv), (xsend, xrecv)
    total = layers * tiles
    lag_z, lag_y, lag_x = 2, 4, 5
    ahead = acts.shape[0] - 1
    assert lag_x <= tiles - 1

    def place(item):
        turn, p = item // tiles, lax.rem(item, tiles)
        tile = (tiles - 1 - p) + me * (2 * p - tiles + 1)
        return layers - 1 - turn, turn, p, tile, lax.rem(turn, 2)

    def fetch(item):
        layer, turn, p, tile, slot = place(item)
        ring = lax.rem(item, ahead + 1)
        return pltpu.make_async_copy(a3_hbm.at[layer, :, :, lane_ds(tile)], acts.at[ring], act_sem.at[ring])

    def load(tile):
        return pltpu.make_async_copy(g_hbm.at[:, :, lane_ds(tile)], grad.at[:, :, lane_ds(tile)], in_sem.at[tile])

    def put(tile):
        return pltpu.make_async_copy(grad.at[:, :, lane_ds(tile)], go_hbm.at[:, :, lane_ds(tile)], out_sem.at[tile])

    def y_at(slot, tile):
        return y_flows(links, d2, yr, ysems, slot, tile)

    def z_at(slot, tile):
        return z_flows(links, zs, zr, zsems, slot, tile)

    def x_at(slot):
        return links.x_edge(d1, xh, xsems, slot, lanes)

    rounds = []
    for name, size in sizes.items():
        bit = 1
        while bit < size:
            rounds.append((name, bit))
            bit *= 2
    assert len(rounds) <= lag_x

    def share(index):
        name, bit = rounds[index]
        pos = links.pos[name]
        other = pos + bit - 2 * bit * lax.rem(pos // bit, 2)
        return pltpu.make_async_remote_copy(sums, gathered.at[index], gsend.at[index], grecv.at[index], device_id={name: other}, device_id_type=MESH)

    def finish(index):
        share(index).wait_send()
        share(index).wait_recv()
        sums[...] = sums[...] + gathered[index]

    for item in range(ahead):
        fetch(item).start()
        load(place(item)[3]).start()
    for item in range(ahead, tiles):
        load(place(item)[3]).start()
    links.zero_edges('gy', yr)
    links.zero_edges('gz', zr)
    links.barrier()

    @pl.loop(0, total + lag_x)
    def _(step):
        @pl.when((step >= lag_z) & (step < total + lag_z))
        def _():
            layer, turn, p, tile, slot = place(step - lag_z)
            cols = lane_ds(tile)

            @pl.when(turn > 0)
            def _():
                links.wait_send(y_at(1 - slot, tile))

            links.wait_recv(z_at(slot, tile))

            def emit(g, out):
                d2[pl.ds(g * ysub, ysub), :, cols] = out

            z_stage(d3, zr, lz, layer, slot, tile, ysub, emit)
            links.start(y_at(slot, tile))

        @pl.when((step >= lag_y) & (step < total + lag_y))
        def _():
            layer, turn, p, tile, slot = place(step - lag_y)
            cols = lane_ds(tile)
            links.wait_recv(y_at(slot, tile))

            def emit(g, zb, side, out):
                d1[pl.ds(g * group, group), pl.ds(zb * ROWS, ROWS), cols] = out.reshape(group, ROWS, TILE)

            y_stage(d2, yr, ly, layer, slot, tile, False, emit)
            pl.when(p == 0)(x_at(slot).start)

        @pl.when(step >= lag_x)
        def _():
            layer, turn, p, tile, slot = place(step - lag_x)
            cols = lane_ds(tile)

            def before_edge():
                x_at(slot).wait_recv()
                x_at(slot).wait_send()

            def emit(y, count, out):
                rows = pl.ds(y, count)
                old = grad[rows, :, cols].astype(F32).reshape(count * nz, TILE)
                grad[rows, :, cols] = (old + out).astype(BF16).reshape(count, nz, TILE)

            x_stage(d1, xh, wx, me, layer, slot, tile, p == tiles - 1, p == 0, before_edge, emit)
            pl.when(layer == 0)(put(tile).start)

        @pl.when(step < total)
        def _():
            layer, turn, p, tile, slot = place(step)
            cols = lane_ds(tile)
            ring = lax.rem(step, ahead + 1)
            fetch(step).wait()

            @pl.when(step + ahead < total)
            def _():
                fetch(step + ahead).start()

            @pl.when(turn == 0)
            def _():
                load(tile).wait()

            @pl.when(turn > 0)
            def _():
                links.wait_send(z_at(1 - slot, tile))

            @pl.when(p == 0)
            def _():
                dw[...] = jnp.zeros_like(dw)
                db[...] = jnp.zeros_like(db)

            span = ysub * nz
            totals = jnp.zeros((8, TILE), F32)
            for g in range(ny // ysub):
                rows = pl.ds(g * ysub, ysub)
                pre = dot(acts[ring, rows].reshape(span, TILE), wd[layer]) + bias[layer]
                cot = grad[rows, :, cols].astype(F32).reshape(span, TILE)
                root = pre * INV_SQRT2
                bell = jnp.exp(-(root * root))
                scaled = (0.5 * cot) * ((1.0 + lax.erf(root)) + (root * TWO_INV_SQRT_PI) * bell)
                totals = totals + jnp.sum(scaled.reshape(span // 8, 8, TILE), axis=0)
                sb[pl.ds(g * span, span), :] = scaled.astype(BF16)
            db[...] += totals
            for g in range(ny // ysub):
                mixed = dot(sb[pl.ds(g * span, span), :], wt[layer]).astype(BF16)
                d3[pl.ds(g * ysub, ysub), :, cols] = mixed.reshape(ysub, nz, TILE)
                planes = dot(pick[...], mixed).astype(BF16)
                zs[0, g, :, cols] = planes[:ROWS]
                zs[1, g, :, cols] = planes[ROWS:]
            links.start(z_at(slot, tile))
            dw[...] += lax.dot_general(acts[ring].reshape(ny * nz, TILE), sb[...], (((0,), (0,)), ((), ())), preferred_element_type=F32)

            @pl.when(p == tiles - 1)
            def _():
                lane = lax.broadcasted_iota(jnp.int32, (chans, TILE), 1) // chans
                diag = jnp.zeros((chans, TILE), F32)
                for i in range(TILE // chans):
                    diag = diag + jnp.where(lane == i, dw[pl.ds(i * chans, chans), :], 0.0)
                sums[layer, pl.ds(0, chans), :] = diag
                sums[layer, pl.ds(chans, 8), :] = db[...]

        for index in range(len(rounds)):
            @pl.when(step == total + index)
            def _():
                if index > 0:
                    finish(index - 1)
                share(index).start()

    finish(len(rounds) - 1)

    @pl.loop(0, tiles)
    def _(tile):
        slot = (layers - 1) % 2
        links.wait_send(y_at(slot, tile))
        links.wait_send(z_at(slot, tile))
        put(tile).wait()


def link_sems(tiles):
    dma = pltpu.SemaphoreType.DMA
    return [dma, dma((2,)), dma((2, tiles)), dma((2, 2, tiles)), dma((2, tiles)), dma((2, 2, tiles))]


def solution(mesh):
    names = ('gx', 'gy', 'gz')
    sizes = {name: mesh.shape[name] for name in names}
    vol_spec = P('dp', 'gx', 'gy', 'gz')
    any_spec = pl.BlockSpec(memory_space=pl.ANY)
    vmem_spec = pl.BlockSpec(memory_space=pltpu.VMEM)
    dma = pltpu.SemaphoreType.DMA

    def local_step(volume, cot_out, filter_taps, w_mix, b_mix):
        chans, nx, ny, nz = volume.shape
        layers, _, num_taps = filter_taps.shape
        half = (num_taps - 1) // 2
        lanes = nx * chans
        tiles = lanes // TILE
        reps = TILE // chans
        ysub = (ROWS - 2 * half) // 2
        params = functools.partial(pltpu.CompilerParams, has_side_effects=True, vmem_limit_bytes=VMEM_BYTES)
        wx_f, wx_b, ly_f, ly_b, lz_f, lz_b, wd, wt = band_weights(filter_taps, w_mix, ysub, nz)
        pick = pick_matrix(half, ysub, nz)
        bias = jnp.tile(b_mix, (1, reps))[:, None, :]

        full = pltpu.VMEM((ny, nz, lanes), BF16)
        one = (ny, nz, TILE)
        two = pltpu.VMEM((2,) + one, BF16)
        y_halo = pltpu.VMEM((2, 2, half, nz, lanes), BF16)
        z_send = pltpu.VMEM((2, ny // ysub, ROWS, lanes), BF16)
        z_halo = pltpu.VMEM((2, 2, ny // ysub, ROWS, lanes), BF16)

        acts = pl.pallas_call(
            functools.partial(fwd_kernel, half, sizes),
            out_shape=jax.ShapeDtypeStruct((layers, ny, nz, lanes), BF16),
            in_specs=[any_spec] + [vmem_spec] * 5,
            out_specs=any_spec,
            scratch_shapes=[full, two, full, y_halo, full, z_send, z_halo, full, dma((tiles,)), dma((tiles,))] + link_sems(tiles),
            compiler_params=params(collective_id=0),
            name='fwd_layers',
        )(to_dense(volume), wx_f, ly_f, lz_f, wd, bias)
        rounds = sum((size - 1).bit_length() for size in sizes.values())
        sum_shape = (layers, chans + 8, TILE)
        grad, sums = pl.pallas_call(
            functools.partial(bwd_kernel, half, sizes, chans),
            out_shape=[jax.ShapeDtypeStruct((ny, nz, lanes), BF16), jax.ShapeDtypeStruct(sum_shape, F32)],
            in_specs=[any_spec] * 2 + [vmem_spec] * 7,
            out_specs=[any_spec, vmem_spec],
            scratch_shapes=[pltpu.VMEM((3,) + one, BF16), full, pltpu.VMEM((ny * nz, TILE), BF16), full, z_send, z_halo, full, y_halo, full, two]
            + [pltpu.VMEM((TILE, TILE), F32), pltpu.VMEM((8, TILE), F32), pltpu.VMEM((rounds,) + sum_shape, F32)]
            + [dma((3,)), dma((tiles,)), dma((tiles,)), dma((rounds,)), dma((rounds,))]
            + link_sems(tiles),
            compiler_params=params(collective_id=1),
            name='bwd_layers',
        )(acts, to_dense(cot_out), wx_b, ly_b, lz_b, pick, wd, wt, bias)
        blocks = sums.reshape(layers, chans + 8, reps, chans).sum(axis=2)
        return from_dense(grad, chans), blocks[:, :chans], blocks[:, chans:].sum(axis=1)

    return jax.shard_map(local_step, mesh=mesh, in_specs=(vol_spec, vol_spec, P(), P(), P()), out_specs=(vol_spec, P('dp'), P('dp')), check_vma=False)
```

```python
import functools

import jax
import jax.numpy as jnp
import numpy as np
from jax import lax
from jax.experimental import pallas as pl
from jax.experimental.pallas import tpu as pltpu
from jax.sharding import PartitionSpec as P

MESH = pl.DeviceIdType.MESH
TILE = 256
ROWS = 16
LANE = 128
SUB = 8
VMEM_BYTES = 60 * 1024 * 1024
INV_SQRT2 = 0.7071067811865476
NEG_LOG2E = -1.4426950408889634
TWO_INV_SQRT_PI = 1.1283791670955126
F32 = jnp.float32
BF16 = jnp.bfloat16


def valid_index(index, keep, num_taps):
    return np.where(keep & (index >= 0) & (index < num_taps), index, -1).astype(np.int32)


def grid2(rows, cols):
    return np.arange(rows)[:, None], np.arange(cols)[None, :]


def x_index(num_taps, chans):
    r, n = grid2(3 * TILE, TILE)
    index = r // chans - TILE // chans - n // chans + num_taps // 2
    return valid_index(index, r % chans == n % chans, num_taps)


def y_index(num_taps):
    half = num_taps // 2
    group = ROWS - 2 * half
    r, k = grid2(group * ROWS, ROWS * ROWS)
    yi, zi = k // ROWS, k % ROWS
    parts = [valid_index(yi - r // ROWS, r % ROWS == zi, num_taps)]
    r, k = grid2(2 * ROWS, ROWS * ROWS)
    q = r % ROWS
    yo = r // ROWS * (group // 2) + q // half
    for first in (0, ROWS - half):
        keep = (q % half + first == zi) & (q < (group // 2) * half)
        parts.append(valid_index(yi - yo, keep, num_taps))
    return np.concatenate(parts, axis=0)


def z_index(num_taps, ysub, nz):
    half = num_taps // 2
    r, k = grid2(ysub * nz, ysub * nz + 2 * ROWS)
    yo, zo = r // nz, r % nz
    is_main = k < ysub * nz
    q = (k - ysub * nz) % ROWS
    low = k < ysub * nz + ROWS
    yi = np.where(is_main, k // nz, q // half)
    zi = np.where(is_main, k % nz, np.where(low, q % half - half, nz + q % half))
    keep = (yi == yo) & (is_main | (q < ysub * half))
    return valid_index(zi - zo + half, keep, num_taps)


def pick_matrix(half, ysub, nz):
    r, k = grid2(2 * ROWS, ysub * nz)
    q = r % ROWS
    zo = q % half + np.where(r < ROWS, 0, nz - half)
    hit = (k // nz == q // half) & (k % nz == zo) & (q < ysub * half)
    return jnp.asarray(hit, BF16)


def band_kernel(taps, wmix, spread, same, xi, yi, zi, xf, xb, yf, yb, zf, zb, wd, wt):
    layers, _, num_taps = taps.shape
    reps = TILE // spread.shape[0]
    for axis, index, fwd, bwd in ((0, xi, xf, xb), (1, yi, yf, yb), (2, zi, zf, zb)):
        @pl.loop(0, index.shape[0] // ROWS)
        def _(chunk):
            rows = pl.ds(pl.multiple_of(chunk * ROWS, ROWS), ROWS)
            which = index[rows, :]
            zero = jnp.zeros(which.shape, F32)
            out = [[zero] * layers, [zero] * layers]
            for t in range(num_taps):
                hit = which == t
                for layer in range(layers):
                    out[0][layer] = jnp.where(hit, taps[layer, axis, t], out[0][layer])
                    out[1][layer] = jnp.where(hit, taps[layer, axis, num_taps - 1 - t], out[1][layer])
            for layer in range(layers):
                fwd[layer, rows, :] = out[0][layer].astype(BF16)
                bwd[layer, rows, :] = out[1][layer].astype(BF16)
    for layer in range(layers):
        for dst, axis in ((wd, 1), (wt, 0)):
            wide = lax.dot_general(wmix[layer], spread[...], (((axis,), (0,)), ((), ())), preferred_element_type=F32)
            full = jnp.concatenate([wide] * reps, axis=0)
            dst[layer] = jnp.where(same[...] != 0, full, 0.0).astype(BF16)


def band_weights(filter_taps, w_mix, ysub, nz):
    layers, _, num_taps = filter_taps.shape
    chans = w_mix.shape[1]
    r, n = grid2(TILE, TILE)
    spread = jnp.asarray(r[:chans] == n % chans, BF16)
    same = jnp.asarray(r // chans == n // chans, jnp.int32)
    indices = [x_index(num_taps, chans), y_index(num_taps), z_index(num_taps, ysub, nz)]
    vmem_spec = pl.BlockSpec(memory_space=pltpu.VMEM)
    shapes = [i.shape for i in indices for _ in range(2)] + [(TILE, TILE)] * 2
    return pl.pallas_call(
        band_kernel,
        out_shape=[jax.ShapeDtypeStruct((layers,) + shape, BF16) for shape in shapes],
        in_specs=[pl.BlockSpec(memory_space=pltpu.SMEM)] + [vmem_spec] * 6,
        out_specs=[vmem_spec] * 8,
        name='band_weights',
    )(filter_taps, w_mix, spread, same, *[jnp.asarray(i) for i in indices])


def entry_kernel(src, dst, rows):
    chans, nx, sub, nz = src.shape

    @pl.loop(0, nx)
    def _(x):
        part = src[:, x].astype(F32).reshape(chans * sub, nz)
        rows[pl.ds(pl.multiple_of(x * chans * sub, chans * sub), chans * sub), :] = part

    eye = (lax.broadcasted_iota(jnp.int32, (nz, nz), 0) == lax.broadcasted_iota(jnp.int32, (nz, nz), 1)).astype(BF16)

    @pl.loop(0, nx * chans // TILE)
    def _(tile):
        for y in range(sub):
            block = rows[pl.ds(tile * TILE * sub + y, TILE, stride=sub), :].astype(BF16)
            out = lax.dot_general(eye, block, (((1,), (1,)), ((), ())), preferred_element_type=F32)
            dst[y, :, lane_ds(tile)] = out.astype(BF16)


def to_dense(a):
    chans, nx, ny, nz = a.shape
    lanes = nx * chans
    return pl.pallas_call(
        entry_kernel,
        grid=(ny // SUB,),
        in_specs=[pl.BlockSpec((chans, nx, SUB, nz), lambda i: (0, 0, i, 0))],
        out_specs=pl.BlockSpec((SUB, nz, lanes), lambda i: (i, 0, 0)),
        out_shape=jax.ShapeDtypeStruct((ny, nz, lanes), BF16),
        scratch_shapes=[pltpu.VMEM((lanes * SUB, nz), F32)],
        compiler_params=pltpu.CompilerParams(vmem_limit_bytes=VMEM_BYTES),
        name='to_dense',
    )(a)


def leave_kernel(src, dst, rows):
    sub, nz, lanes = src.shape
    chans, nx = dst.shape[:2]
    eye = (lax.broadcasted_iota(jnp.int32, (TILE, TILE), 0) == lax.broadcasted_iota(jnp.int32, (TILE, TILE), 1)).astype(BF16)
    pad = jnp.zeros((LANE - nz, TILE), BF16)

    @pl.loop(0, lanes // TILE)
    def _(tile):
        for y in range(0, sub, 2):
            block = jnp.concatenate([src[y, :, lane_ds(tile)], pad, src[y + 1, :, lane_ds(tile)], pad], axis=0)
            out = lax.dot_general(eye, block, (((1,), (1,)), ((), ())), preferred_element_type=F32)
            rows[pl.ds(tile * TILE * sub + y, TILE, stride=sub), :] = out[:, :LANE]
            rows[pl.ds(tile * TILE * sub + y + 1, TILE, stride=sub), :] = out[:, LANE:]

    @pl.loop(0, nx)
    def _(x):
        part = rows[pl.ds(pl.multiple_of(x * chans * sub, chans * sub), chans * sub), :]
        dst[:, x] = part[:, :nz].astype(BF16).reshape(chans, sub, nz)


def from_dense(a, chans):
    ny, nz, lanes = a.shape
    nx = lanes // chans
    return pl.pallas_call(
        leave_kernel,
        grid=(ny // SUB,),
        in_specs=[pl.BlockSpec((SUB, nz, lanes), lambda i: (i, 0, 0))],
        out_specs=pl.BlockSpec((chans, nx, SUB, nz), lambda i: (0, 0, i, 0)),
        out_shape=jax.ShapeDtypeStruct((chans, nx, ny, nz), BF16),
        scratch_shapes=[pltpu.VMEM((lanes * SUB, LANE), F32)],
        compiler_params=pltpu.CompilerParams(vmem_limit_bytes=VMEM_BYTES),
        name='from_dense',
    )(a)


def dims(shape, half):
    ny, nz, lanes = shape
    group = ROWS - 2 * half
    return ny, nz, lanes, lanes // TILE, group, group // 2


def lane_ds(tile):
    return pl.ds(pl.multiple_of(tile * TILE, TILE), TILE)


class Links:
    def __init__(self, sizes):
        self.sizes = sizes
        self.pos = {name: lax.axis_index(name) for name in ('gx', 'gy', 'gz')}

    def barrier(self):
        sem = pltpu.get_barrier_semaphore()
        count = 0
        for name, size in self.sizes.items():
            for step in range(1, size):
                pl.semaphore_signal(sem, inc=1, device_id={name: lax.rem(self.pos[name] + step, size)}, device_id_type=MESH)
                count += 1
        pl.semaphore_wait(sem, count)

    def pair(self, name, low_src, high_src, dst, sems, slot, tile):
        send, recv = sems
        pos, size = self.pos[name], self.sizes[name]
        down = pltpu.make_async_remote_copy(low_src, dst[1], send.at[0, tile], recv.at[slot, 0, tile], device_id={name: jnp.maximum(pos - 1, 0)}, device_id_type=MESH)
        up = pltpu.make_async_remote_copy(high_src, dst[0], send.at[1, tile], recv.at[slot, 1, tile], device_id={name: jnp.minimum(pos + 1, size - 1)}, device_id_type=MESH)
        return (down, pos > 0), (up, pos < size - 1)

    def start(self, flows):
        for copy, has in flows:
            pl.when(has)(copy.start)

    def wait_recv(self, flows):
        (down, has_low), (up, has_high) = flows
        pl.when(has_high)(down.wait_recv)
        pl.when(has_low)(up.wait_recv)

    def wait_send(self, flows):
        for copy, has in flows:
            pl.when(has)(copy.wait_send)

    def zero_edges(self, name, halos):
        for side, at in ((0, 0), (1, self.sizes[name] - 1)):
            @pl.when(self.pos[name] == at)
            def _():
                for slot in range(2):
                    halos[slot, side] = jnp.zeros(halos.shape[2:], halos.dtype)

    def x_edge(self, src, xh, sems, slot, lanes):
        send, recv = sems
        me = self.pos['gx']
        first = pl.multiple_of((1 - me) * (lanes - TILE), TILE)
        return pltpu.make_async_remote_copy(src.at[:, :, pl.ds(first, TILE)], xh.at[slot], send, recv.at[slot], device_id={'gx': 1 - me}, device_id_type=MESH)


def y_flows(links, buf, halos, sems, slot, tile):
    cols = lane_ds(tile)
    ny, half = buf.shape[0], halos.shape[2]
    dst = [halos.at[slot, side, :, :, cols] for side in range(2)]
    return links.pair('gy', buf.at[pl.ds(0, half), :, cols], buf.at[pl.ds(ny - half, half), :, cols], dst, sems, slot, tile)


def z_flows(links, zs, zr, sems, slot, tile):
    cols = lane_ds(tile)
    dst = [zr.at[slot, side, :, :, cols] for side in range(2)]
    return links.pair('gz', zs.at[0, :, :, cols], zs.at[1, :, :, cols], dst, sems, slot, tile)


def dot(a, b):
    return jnp.dot(a, b, preferred_element_type=F32)


def x_stage(src, xh, wx, me, layer, slot, tile, outer, edge, before_edge, emit):
    ny, nz, lanes = src.shape
    count = 8
    far, near = lanes - 2 * TILE, 0

    def rows(y, lane, width, weight):
        block = src[pl.ds(y, count), :, pl.ds(pl.multiple_of(lane, TILE), width)]
        return dot(block.reshape(count * nz, width), weight)

    @pl.when(outer)
    def _():
        weight = wx[layer, pl.ds(pl.multiple_of((1 - me) * TILE, TILE), 2 * TILE), :]
        for y in range(0, ny, count):
            emit(y, count, rows(y, me * far, 2 * TILE, weight))

    @pl.when(jnp.logical_not(outer | edge))
    def _():
        weight = wx[layer]
        for y in range(0, ny, count):
            emit(y, count, rows(y, (tile - 1) * TILE, 3 * TILE, weight))

    @pl.when(edge)
    def _():
        before_edge()
        weight = wx[layer, pl.ds(pl.multiple_of(me * TILE, TILE), 2 * TILE), :]
        other = wx[layer, pl.ds(pl.multiple_of((1 - me) * 2 * TILE, TILE), TILE), :]
        for y in range(0, ny, count):
            outside = dot(xh[slot, pl.ds(y, count)].reshape(count * nz, TILE), other)
            emit(y, count, rows(y, (1 - me) * far, 2 * TILE, weight) + outside)


def y_stage(src, halos, ly, layer, slot, tile, picks, emit):
    ny, nz, lanes, tiles, group, ysub = dims(src.shape, halos.shape[2])
    half = halos.shape[2]
    cols = lane_ds(tile)
    main = group * ROWS
    base = ly[layer, pl.ds(0, main), :]
    low = ly[layer, pl.ds(0, main + 2 * ROWS), :]
    high = jnp.concatenate([base, ly[layer, pl.ds(main + 2 * ROWS, 2 * ROWS), :]], axis=0)
    for g in range(ny // group):
        for zb in range(nz // ROWS):
            zrows = pl.ds(zb * ROWS, ROWS)
            first, last = g * group - half, g * group - half + ROWS
            parts = []
            if first < 0:
                parts.append(halos[slot, 0, :, zrows, cols])
            parts.append(src[pl.ds(max(first, 0), min(last, ny) - max(first, 0)), zrows, cols])
            if last > ny:
                parts.append(halos[slot, 1, :, zrows, cols])
            rhs = jnp.concatenate(parts, axis=0) if len(parts) > 1 else parts[0]
            side = {0: 0, nz // ROWS - 1: 1}.get(zb) if picks else None
            lhs = {None: base, 0: low, 1: high}[side]
            emit(g, zb, side, dot(lhs, rhs.reshape(ROWS * ROWS, TILE)).astype(BF16))


def z_stage(src, zr, lz, layer, slot, tile, ysub, emit):
    ny, nz, lanes = src.shape
    cols = lane_ds(tile)
    lhs = lz[layer]
    for g in range(ny // ysub):
        main = src[pl.ds(g * ysub, ysub), :, cols].reshape(ysub * nz, TILE)
        rhs = jnp.concatenate([main, zr[slot, 0, g, :, cols], zr[slot, 1, g, :, cols]], axis=0)
        emit(g, dot(lhs, rhs).astype(BF16).reshape(ysub, nz, TILE))


def fwd_kernel(half, sizes, v_hbm, wx, ly, lz, wd, bias, a3_hbm, vol, xh, a1, yr, a2, zs, zr, a3, in_sem, out_sem, xsend, xrecv, ysend, yrecv, zsend, zrecv):
    ny, nz, lanes, tiles, group, ysub = dims(v_hbm.shape, half)
    layers = wx.shape[0]
    links = Links(sizes)
    me = links.pos['gx']
    ysems, zsems, xsems = (ysend, yrecv), (zsend, zrecv), (xsend, xrecv)
    total = layers * tiles
    lag_y, lag_z = 2, 4
    assert lag_z <= tiles - 2

    def place(item):
        layer, p = item // tiles, lax.rem(item, tiles)
        return layer, p, p + me * (tiles - 1 - 2 * p), lax.rem(layer, 2)

    def fetch(tile):
        return pltpu.make_async_copy(v_hbm.at[:, :, lane_ds(tile)], vol.at[:, :, lane_ds(tile)], in_sem.at[tile])

    def put(layer, tile):
        return pltpu.make_async_copy(a3.at[:, :, lane_ds(tile)], a3_hbm.at[layer, :, :, lane_ds(tile)], out_sem.at[tile])

    def y_at(slot, tile):
        return y_flows(links, a1, yr, ysems, slot, tile)

    def z_at(slot, tile):
        return z_flows(links, zs, zr, zsems, slot, tile)

    def x_at(slot):
        return links.x_edge(vol, xh, xsems, slot, lanes)

    edge_tile = place(tiles - 1)[2]
    fetch(edge_tile).start()
    for p in range(tiles - 1):
        fetch(place(p)[2]).start()
    links.zero_edges('gy', yr)
    links.zero_edges('gz', zr)
    links.barrier()
    fetch(edge_tile).wait()
    x_at(0).start()

    @pl.loop(0, total + lag_z)
    def _(step):
        @pl.when(step < total)
        def _():
            layer, p, tile, slot = place(step)

            @pl.when(layer == 0)
            def _():
                pl.when(p == 0)(fetch(tile).wait)
                pl.when(p < tiles - 2)(fetch(place(p + 1)[2]).wait)

            @pl.when(layer > 0)
            def _():
                links.wait_send(y_at(1 - slot, tile))

            def before_edge():
                x_at(slot).wait_recv()
                x_at(slot).wait_send()

            def emit(y, count, out):
                a1[pl.ds(y, count), :, lane_ds(tile)] = out.astype(BF16).reshape(count, nz, TILE)

            x_stage(vol, xh, wx, me, layer, slot, tile, p == 0, p == tiles - 1, before_edge, emit)
            links.start(y_at(slot, tile))

        @pl.when((step >= lag_y) & (step < total + lag_y))
        def _():
            layer, p, tile, slot = place(step - lag_y)
            cols = lane_ds(tile)

            @pl.when(layer > 0)
            def _():
                links.wait_send(z_at(1 - slot, tile))

            links.wait_recv(y_at(slot, tile))

            def emit(g, zb, side, out):
                a2[pl.ds(g * group, group), pl.ds(zb * ROWS, ROWS), cols] = out[: group * ROWS].reshape(group, ROWS, TILE)
                if side is not None:
                    zs[side, pl.ds(2 * g, 2), :, cols] = out[group * ROWS :].reshape(2, ROWS, TILE)

            y_stage(a1, yr, ly, layer, slot, tile, True, emit)
            links.start(z_at(slot, tile))

        @pl.when(step >= lag_z)
        def _():
            layer, p, tile, slot = place(step - lag_z)
            cols = lane_ds(tile)

            @pl.when(layer > 0)
            def _():
                put(layer - 1, tile).wait()

            links.wait_recv(z_at(slot, tile))

            groups = ny // ysub

            def emit(g, out):
                a3[pl.ds(g * ysub, ysub), :, cols] = out

            @pl.when(layer == layers - 1)
            def _():
                z_stage(a2, zr, lz, layer, slot, tile, ysub, emit)

            @pl.when(layer < layers - 1)
            def _():
                held = {}

                def mix_and_update(g, out):
                    if out is not None:
                        emit(g, out)
                        held[g] = dot(out.reshape(ysub * nz, TILE), wd[layer])
                    if g >= 1:
                        mix = held.pop(g - 1)
                        for i in range(ysub):
                            y = (g - 1) * ysub + i
                            pre = mix[i * nz : (i + 1) * nz] + bias[layer]
                            new = vol[y, :, cols].astype(F32) + (0.5 * pre) * (1.0 + lax.erf(pre * INV_SQRT2))
                            vol[y, :, cols] = new.astype(BF16)

                z_stage(a2, zr, lz, layer, slot, tile, ysub, mix_and_update)
                mix_and_update(groups, None)
                pl.when(p == tiles - 1)(x_at(1 - slot).start)

            put(layer, tile).start()

    @pl.loop(0, tiles)
    def _(tile):
        slot = (layers - 1) % 2
        links.wait_send(y_at(slot, tile))
        links.wait_send(z_at(slot, tile))
        put(layers - 1, tile).wait()


def bwd_kernel(half, sizes, chans, a3_hbm, g_hbm, wx, ly, lz, pick, wd, wt, bias, go_hbm, sums, acts, grad, sb, d3, zs, zr, d2, yr, d1, xh, dw, db, gathered, act_sem, in_sem, out_sem, gsend, grecv, xsend, xrecv, ysend, yrecv, zsend, zrecv):
    ny, nz, lanes, tiles, group, ysub = dims(g_hbm.shape, half)
    layers = wx.shape[0]
    links = Links(sizes)
    me = links.pos['gx']
    ysems, zsems, xsems = (ysend, yrecv), (zsend, zrecv), (xsend, xrecv)
    total = layers * tiles
    lag_z, lag_y, lag_x = 2, 5, 6
    ahead = acts.shape[0] - 1
    assert lag_x <= tiles

    def place(item):
        turn, p = item // tiles, lax.rem(item, tiles)
        tile = (tiles - 1 - p) + me * (2 * p - tiles + 1)
        return layers - 1 - turn, turn, p, tile, lax.rem(turn, 2)

    def fetch(item):
        layer, turn, p, tile, slot = place(item)
        ring = lax.rem(item, ahead + 1)
        return pltpu.make_async_copy(a3_hbm.at[layer, :, :, lane_ds(tile)], acts.at[ring], act_sem.at[ring])

    def load(tile):
        return pltpu.make_async_copy(g_hbm.at[:, :, lane_ds(tile)], grad.at[:, :, lane_ds(tile)], in_sem.at[tile])

    def put(tile):
        return pltpu.make_async_copy(grad.at[:, :, lane_ds(tile)], go_hbm.at[:, :, lane_ds(tile)], out_sem.at[tile])

    def y_at(slot, tile):
        return y_flows(links, d2, yr, ysems, slot, tile)

    def z_at(slot, tile):
        return z_flows(links, zs, zr, zsems, slot, tile)

    def x_at(slot):
        return links.x_edge(d1, xh, xsems, slot, lanes)

    rounds = []
    for name, size in sizes.items():
        bit = 1
        while bit < size:
            rounds.append((name, bit))
            bit *= 2
    assert len(rounds) <= lag_x

    def share(index):
        name, bit = rounds[index]
        pos = links.pos[name]
        other = pos + bit - 2 * bit * lax.rem(pos // bit, 2)
        return pltpu.make_async_remote_copy(sums, gathered.at[index], gsend.at[index], grecv.at[index], device_id={name: other}, device_id_type=MESH)

    def finish(index):
        share(index).wait_send()
        share(index).wait_recv()
        sums[...] = sums[...] + gathered[index]

    for item in range(ahead):
        fetch(item).start()
        load(place(item)[3]).start()
    for item in range(ahead, tiles):
        load(place(item)[3]).start()
    links.zero_edges('gy', yr)
    links.zero_edges('gz', zr)
    links.barrier()

    @pl.loop(0, total + lag_x)
    def _(step):
        @pl.when((step >= lag_y) & (step < total + lag_y))
        def _():
            layer, turn, p, tile, slot = place(step - lag_y)
            cols = lane_ds(tile)
            links.wait_recv(y_at(slot, tile))

            def emit(g, zb, side, out):
                d1[pl.ds(g * group, group), pl.ds(zb * ROWS, ROWS), cols] = out.reshape(group, ROWS, TILE)

            y_stage(d2, yr, ly, layer, slot, tile, False, emit)
            pl.when(p == 0)(x_at(slot).start)

        @pl.when(step >= lag_x)
        def _():
            layer, turn, p, tile, slot = place(step - lag_x)
            cols = lane_ds(tile)

            def before_edge():
                x_at(slot).wait_recv()
                x_at(slot).wait_send()

            def emit(y, count, out):
                rows = pl.ds(y, count)
                old = grad[rows, :, cols].astype(F32).reshape(count * nz, TILE)
                grad[rows, :, cols] = (old + out).astype(BF16).reshape(count, nz, TILE)

            x_stage(d1, xh, wx, me, layer, slot, tile, p == tiles - 1, p == 0, before_edge, emit)
            pl.when(layer == 0)(put(tile).start)

        @pl.when(step < total)
        def _():
            layer, turn, p, tile, slot = place(step)
            cols = lane_ds(tile)
            ring = lax.rem(step, ahead + 1)
            fetch(step).wait()

            @pl.when(step + ahead < total)
            def _():
                fetch(step + ahead).start()

            @pl.when(turn == 0)
            def _():
                load(tile).wait()

            @pl.when(turn > 0)
            def _():
                links.wait_send(z_at(1 - slot, tile))

            @pl.when(p == 0)
            def _():
                dw[...] = jnp.zeros_like(dw)
                db[...] = jnp.zeros_like(db)

            span = ysub * nz
            groups = ny // ysub

            def mix_of(g):
                return dot(acts[ring, pl.ds(g * ysub, ysub)].reshape(span, TILE), wd[layer])

            totals = jnp.zeros((8, TILE), F32)
            mix, mixed = mix_of(0), {}
            for g in range(groups + 2):
                following = mix_of(g + 1) if g + 1 < groups else None
                if 1 <= g <= groups:
                    mixed[g - 1] = dot(sb[pl.ds((g - 1) * span, span), :], wt[layer]).astype(BF16)
                    d3[pl.ds((g - 1) * ysub, ysub), :, cols] = mixed[g - 1].reshape(ysub, nz, TILE)
                if g >= 2:
                    planes = dot(pick[...], mixed.pop(g - 2)).astype(BF16)
                    zs[0, g - 2, :, cols] = planes[:ROWS]
                    zs[1, g - 2, :, cols] = planes[ROWS:]
                if g < groups:
                    for i in range(ysub):
                        y = g * ysub + i
                        pre = mix[i * nz : (i + 1) * nz] + bias[layer]
                        cot = grad[y, :, cols].astype(F32)
                        root = pre * INV_SQRT2
                        bell = jnp.exp2((root * root) * NEG_LOG2E)
                        scaled = (0.5 * cot) * ((1.0 + lax.erf(root)) + (root * TWO_INV_SQRT_PI) * bell)
                        totals = totals + jnp.sum(scaled.reshape(nz // 8, 8, TILE), axis=0)
                        sb[pl.ds(y * nz, nz), :] = scaled.astype(BF16)
                mix = following
            db[...] += totals
            links.start(z_at(slot, tile))
            dw[...] += lax.dot_general(acts[ring].reshape(ny * nz, TILE), sb[...], (((0,), (0,)), ((), ())), preferred_element_type=F32)

            @pl.when(p == tiles - 1)
            def _():
                lane = lax.broadcasted_iota(jnp.int32, (chans, TILE), 1) // chans
                diag = jnp.zeros((chans, TILE), F32)
                for i in range(TILE // chans):
                    diag = diag + jnp.where(lane == i, dw[pl.ds(i * chans, chans), :], 0.0)
                sums[layer, pl.ds(0, chans), :] = diag
                sums[layer, pl.ds(chans, 8), :] = db[...]

        @pl.when((step >= lag_z) & (step < total + lag_z))
        def _():
            layer, turn, p, tile, slot = place(step - lag_z)
            cols = lane_ds(tile)

            @pl.when(turn > 0)
            def _():
                links.wait_send(y_at(1 - slot, tile))

            links.wait_recv(z_at(slot, tile))

            def emit(g, out):
                d2[pl.ds(g * ysub, ysub), :, cols] = out

            z_stage(d3, zr, lz, layer, slot, tile, ysub, emit)
            links.start(y_at(slot, tile))

        for index in range(len(rounds)):
            @pl.when(step == total + index)
            def _():
                if index > 0:
                    finish(index - 1)
                share(index).start()

    finish(len(rounds) - 1)

    @pl.loop(0, tiles)
    def _(tile):
        slot = (layers - 1) % 2
        links.wait_send(y_at(slot, tile))
        links.wait_send(z_at(slot, tile))
        put(tile).wait()


def link_sems(tiles):
    dma = pltpu.SemaphoreType.DMA
    return [dma, dma((2,)), dma((2, tiles)), dma((2, 2, tiles)), dma((2, tiles)), dma((2, 2, tiles))]


def solution(mesh):
    names = ('gx', 'gy', 'gz')
    sizes = {name: mesh.shape[name] for name in names}
    vol_spec = P('dp', 'gx', 'gy', 'gz')
    any_spec = pl.BlockSpec(memory_space=pl.ANY)
    vmem_spec = pl.BlockSpec(memory_space=pltpu.VMEM)
    dma = pltpu.SemaphoreType.DMA

    def local_step(volume, cot_out, filter_taps, w_mix, b_mix):
        chans, nx, ny, nz = volume.shape
        layers, _, num_taps = filter_taps.shape
        half = (num_taps - 1) // 2
        lanes = nx * chans
        tiles = lanes // TILE
        reps = TILE // chans
        ysub = (ROWS - 2 * half) // 2
        params = functools.partial(pltpu.CompilerParams, has_side_effects=True, vmem_limit_bytes=VMEM_BYTES)
        wx_f, wx_b, ly_f, ly_b, lz_f, lz_b, wd, wt = band_weights(filter_taps, w_mix, ysub, nz)
        pick = pick_matrix(half, ysub, nz)
        bias = jnp.tile(b_mix, (1, reps))[:, None, :]

        full = pltpu.VMEM((ny, nz, lanes), BF16)
        one = (ny, nz, TILE)
        two = pltpu.VMEM((2,) + one, BF16)
        y_halo = pltpu.VMEM((2, 2, half, nz, lanes), BF16)
        z_send = pltpu.VMEM((2, ny // ysub, ROWS, lanes), BF16)
        z_halo = pltpu.VMEM((2, 2, ny // ysub, ROWS, lanes), BF16)

        acts = pl.pallas_call(
            functools.partial(fwd_kernel, half, sizes),
            out_shape=jax.ShapeDtypeStruct((layers, ny, nz, lanes), BF16),
            in_specs=[any_spec] + [vmem_spec] * 5,
            out_specs=any_spec,
            scratch_shapes=[full, two, full, y_halo, full, z_send, z_halo, full, dma((tiles,)), dma((tiles,))] + link_sems(tiles),
            compiler_params=params(collective_id=0),
            name='fwd_layers',
        )(to_dense(volume), wx_f, ly_f, lz_f, wd, bias)
        rounds = sum((size - 1).bit_length() for size in sizes.values())
        sum_shape = (layers, chans + 8, TILE)
        grad, sums = pl.pallas_call(
            functools.partial(bwd_kernel, half, sizes, chans),
            out_shape=[jax.ShapeDtypeStruct((ny, nz, lanes), BF16), jax.ShapeDtypeStruct(sum_shape, F32)],
            in_specs=[any_spec] * 2 + [vmem_spec] * 7,
            out_specs=[any_spec, vmem_spec],
            scratch_shapes=[pltpu.VMEM((3,) + one, BF16), full, pltpu.VMEM((ny * nz, TILE), BF16), full, z_send, z_halo, full, y_halo, full, two]
            + [pltpu.VMEM((TILE, TILE), F32), pltpu.VMEM((8, TILE), F32), pltpu.VMEM((rounds,) + sum_shape, F32)]
            + [dma((3,)), dma((tiles,)), dma((tiles,)), dma((rounds,)), dma((rounds,))]
            + link_sems(tiles),
            compiler_params=params(collective_id=1),
            name='bwd_layers',
        )(acts, to_dense(cot_out), wx_b, ly_b, lz_b, pick, wd, wt, bias)
        blocks = sums.reshape(layers, chans + 8, reps, chans).sum(axis=2)
        return from_dense(grad, chans), blocks[:, :chans], blocks[:, chans:].sum(axis=1)

    return jax.shard_map(local_step, mesh=mesh, in_specs=(vol_spec, vol_spec, P(), P(), P()), out_specs=(vol_spec, P('dp'), P('dp')), check_vma=False)
```

```python
import functools

import jax
import jax.numpy as jnp
import numpy as np
from jax import lax
from jax.experimental import pallas as pl
from jax.experimental.pallas import tpu as pltpu
from jax.sharding import PartitionSpec as P

MESH = pl.DeviceIdType.MESH
TILE = 256
ROWS = 16
LANE = 128
SUB = 8
VMEM_BYTES = 60 * 1024 * 1024
INV_SQRT2 = 0.7071067811865476
NEG_LOG2E = -1.4426950408889634
TWO_INV_SQRT_PI = 1.1283791670955126
F32 = jnp.float32
BF16 = jnp.bfloat16


def valid_index(index, keep, num_taps):
    return np.where(keep & (index >= 0) & (index < num_taps), index, -1).astype(np.int32)


def grid2(rows, cols):
    return np.arange(rows)[:, None], np.arange(cols)[None, :]


def x_index(num_taps, chans):
    x, n = grid2(3 * TILE // chans, TILE)
    index = x - TILE // chans - n // chans + num_taps // 2
    return valid_index(index, n >= 0, num_taps)


def y_index(num_taps):
    half = num_taps // 2
    group = ROWS - 2 * half
    r, k = grid2(group * ROWS, ROWS * ROWS)
    yi, zi = k // ROWS, k % ROWS
    parts = [valid_index(yi - r // ROWS, r % ROWS == zi, num_taps)]
    r, k = grid2(2 * ROWS, ROWS * ROWS)
    q = r % ROWS
    yo = r // ROWS * (group // 2) + q // half
    for first in (0, ROWS - half):
        keep = (q % half + first == zi) & (q < (group // 2) * half)
        parts.append(valid_index(yi - yo, keep, num_taps))
    return np.concatenate(parts, axis=0)


def z_index(num_taps, ysub, nz):
    half = num_taps // 2
    r, k = grid2(ysub * nz, ysub * nz + 2 * ROWS)
    yo, zo = r // nz, r % nz
    is_main = k < ysub * nz
    q = (k - ysub * nz) % ROWS
    low = k < ysub * nz + ROWS
    yi = np.where(is_main, k // nz, q // half)
    zi = np.where(is_main, k % nz, np.where(low, q % half - half, nz + q % half))
    keep = (yi == yo) & (is_main | (q < ysub * half))
    return valid_index(zi - zo + half, keep, num_taps)


def pick_matrix(half, ysub, nz):
    r, k = grid2(2 * ROWS, ysub * nz)
    q = r % ROWS
    zo = q % half + np.where(r < ROWS, 0, nz - half)
    hit = (k // nz == q // half) & (k % nz == zo) & (q < ysub * half)
    return jnp.asarray(hit, BF16)


def band_kernel(taps, wmix, spread, same, xi, yi, zi, xf, xb, yf, yb, zf, zb, wd, wt):
    layers, _, num_taps = taps.shape
    chans = spread.shape[0]
    reps = TILE // chans

    def values(which, axis):
        zero = jnp.zeros(which.shape, F32)
        fwd, bwd = [zero] * layers, [zero] * layers
        for t in range(num_taps):
            hit = which == t
            for layer in range(layers):
                fwd[layer] = jnp.where(hit, taps[layer, axis, t], fwd[layer])
                bwd[layer] = jnp.where(hit, taps[layer, axis, num_taps - 1 - t], bwd[layer])
        return fwd, bwd

    diag = lax.rem(lax.broadcasted_iota(jnp.int32, (chans, TILE), 1), chans) == lax.broadcasted_iota(jnp.int32, (chans, TILE), 0)
    for dst, lines in zip((xf, xb), values(xi[...], 0)):
        for layer in range(layers):
            for x in range(xi.shape[0]):
                line = jnp.broadcast_to(lines[layer][x : x + 1], (chans, TILE))
                dst[layer, pl.ds(x * chans, chans), :] = jnp.where(diag, line, 0.0).astype(BF16)
    for axis, index, fwd, bwd in ((1, yi, yf, yb), (2, zi, zf, zb)):
        @pl.loop(0, index.shape[0] // ROWS)
        def _(chunk):
            rows = pl.ds(pl.multiple_of(chunk * ROWS, ROWS), ROWS)
            out = values(index[rows, :], axis)
            for layer in range(layers):
                fwd[layer, rows, :] = out[0][layer].astype(BF16)
                bwd[layer, rows, :] = out[1][layer].astype(BF16)
    for layer in range(layers):
        for dst, axis in ((wd, 1), (wt, 0)):
            wide = lax.dot_general(wmix[layer], spread[...], (((axis,), (0,)), ((), ())), preferred_element_type=F32)
            full = jnp.concatenate([wide] * reps, axis=0)
            dst[layer] = jnp.where(same[...] != 0, full, 0.0).astype(BF16)


def band_weights(filter_taps, w_mix, ysub, nz):
    layers, _, num_taps = filter_taps.shape
    chans = w_mix.shape[1]
    r, n = grid2(TILE, TILE)
    spread = jnp.asarray(r[:chans] == n % chans, BF16)
    same = jnp.asarray(r // chans == n // chans, jnp.int32)
    indices = [x_index(num_taps, chans), y_index(num_taps), z_index(num_taps, ysub, nz)]
    vmem_spec = pl.BlockSpec(memory_space=pltpu.VMEM)
    shapes = [(3 * TILE, TILE)] * 2 + [i.shape for i in indices[1:] for _ in range(2)] + [(TILE, TILE)] * 2
    return pl.pallas_call(
        band_kernel,
        out_shape=[jax.ShapeDtypeStruct((layers,) + shape, BF16) for shape in shapes],
        in_specs=[pl.BlockSpec(memory_space=pltpu.SMEM)] + [vmem_spec] * 6,
        out_specs=[vmem_spec] * 8,
        name='band_weights',
    )(filter_taps, w_mix, spread, same, *[jnp.asarray(i) for i in indices])


def relayout(src, dst, rows):
    chans, nx, ny, nz = src.shape
    step = ny + SUB
    for c in range(chans):
        for x in range(nx):
            rows[pl.ds((x * chans + c) * step, ny), :] = src[c, x].astype(F32)
    eye = (lax.broadcasted_iota(jnp.int32, (nz, nz), 0) == lax.broadcasted_iota(jnp.int32, (nz, nz), 1)).astype(BF16)

    @pl.loop(0, ny // SUB)
    def _(part):
        for i in range(SUB):
            y = part * SUB + i
            block = rows[pl.ds(y, TILE, stride=step), :].astype(BF16)
            out = lax.dot_general(eye, block, (((1,), (1,)), ((), ())), preferred_element_type=F32)
            dst[y] = out.astype(BF16)


def to_dense(a):
    chans, nx, ny, nz = a.shape
    per = TILE // chans
    return pl.pallas_call(
        relayout,
        grid=(nx // per,),
        in_specs=[pl.BlockSpec((chans, per, ny, nz), lambda i: (0, i, 0, 0))],
        out_specs=pl.BlockSpec((ny, nz, TILE), lambda i: (0, 0, i)),
        out_shape=jax.ShapeDtypeStruct((ny, nz, nx * chans), BF16),
        scratch_shapes=[pltpu.VMEM((TILE * (ny + SUB), nz), F32)],
        compiler_params=pltpu.CompilerParams(vmem_limit_bytes=VMEM_BYTES),
        name='to_dense',
    )(a)


def leave_kernel(src, dst, rows):
    ny, nz, _ = src.shape
    chans, nx = dst.shape[:2]
    step = ny + SUB
    eye = (lax.broadcasted_iota(jnp.int32, (TILE, TILE), 0) == lax.broadcasted_iota(jnp.int32, (TILE, TILE), 1)).astype(BF16)
    pad = jnp.zeros((LANE - nz, TILE), BF16)

    @pl.loop(0, ny // SUB)
    def _(part):
        for i in range(0, SUB, 2):
            y = part * SUB + i
            block = jnp.concatenate([src[y], pad, src[y + 1], pad], axis=0)
            out = lax.dot_general(eye, block, (((1,), (1,)), ((), ())), preferred_element_type=F32)
            rows[pl.ds(y, TILE, stride=step), :] = out[:, :LANE]
            rows[pl.ds(y + 1, TILE, stride=step), :] = out[:, LANE:]

    for c in range(chans):
        for x in range(nx):
            dst[c, x] = rows[pl.ds((x * chans + c) * step, ny), :][:, :nz].astype(BF16)


def from_dense(a, chans):
    ny, nz, lanes = a.shape
    per = TILE // chans
    return pl.pallas_call(
        leave_kernel,
        grid=(lanes // TILE,),
        in_specs=[pl.BlockSpec((ny, nz, TILE), lambda i: (0, 0, i))],
        out_specs=pl.BlockSpec((chans, per, ny, nz), lambda i: (0, i, 0, 0)),
        out_shape=jax.ShapeDtypeStruct((chans, lanes // chans, ny, nz), BF16),
        scratch_shapes=[pltpu.VMEM((TILE * (ny + SUB), LANE), F32)],
        compiler_params=pltpu.CompilerParams(vmem_limit_bytes=VMEM_BYTES),
        name='from_dense',
    )(a)


def dims(shape, half):
    ny, nz, lanes = shape
    group = ROWS - 2 * half
    return ny, nz, lanes, lanes // TILE, group, group // 2


def lane_ds(tile):
    return pl.ds(pl.multiple_of(tile * TILE, TILE), TILE)


class Links:
    def __init__(self, sizes):
        self.sizes = sizes
        self.pos = {name: lax.axis_index(name) for name in ('gx', 'gy', 'gz')}

    def barrier(self):
        sem = pltpu.get_barrier_semaphore()
        count = 0
        for name, size in self.sizes.items():
            for step in range(1, size):
                pl.semaphore_signal(sem, inc=1, device_id={name: lax.rem(self.pos[name] + step, size)}, device_id_type=MESH)
                count += 1
        pl.semaphore_wait(sem, count)

    def pair(self, name, low_src, high_src, dst, sems, slot, tile):
        send, recv = sems
        pos, size = self.pos[name], self.sizes[name]
        down = pltpu.make_async_remote_copy(low_src, dst[1], send.at[0, tile], recv.at[slot, 0, tile], device_id={name: jnp.maximum(pos - 1, 0)}, device_id_type=MESH)
        up = pltpu.make_async_remote_copy(high_src, dst[0], send.at[1, tile], recv.at[slot, 1, tile], device_id={name: jnp.minimum(pos + 1, size - 1)}, device_id_type=MESH)
        return (down, pos > 0), (up, pos < size - 1)

    def start(self, flows):
        for copy, has in flows:
            pl.when(has)(copy.start)

    def wait_recv(self, flows):
        (down, has_low), (up, has_high) = flows
        pl.when(has_high)(down.wait_recv)
        pl.when(has_low)(up.wait_recv)

    def wait_send(self, flows):
        for copy, has in flows:
            pl.when(has)(copy.wait_send)

    def zero_edges(self, name, halos):
        for side, at in ((0, 0), (1, self.sizes[name] - 1)):
            @pl.when(self.pos[name] == at)
            def _():
                for slot in range(2):
                    halos[slot, side] = jnp.zeros(halos.shape[2:], halos.dtype)

    def x_edge(self, src, xh, sems, slot, lanes):
        send, recv = sems
        me = self.pos['gx']
        first = pl.multiple_of((1 - me) * (lanes - TILE), TILE)
        return pltpu.make_async_remote_copy(src.at[:, :, pl.ds(first, TILE)], xh.at[slot], send, recv.at[slot], device_id={'gx': 1 - me}, device_id_type=MESH)


def y_flows(links, buf, halos, sems, slot, tile):
    cols = lane_ds(tile)
    ny, half = buf.shape[0], halos.shape[2]
    dst = [halos.at[slot, side, :, :, cols] for side in range(2)]
    return links.pair('gy', buf.at[pl.ds(0, half), :, cols], buf.at[pl.ds(ny - half, half), :, cols], dst, sems, slot, tile)


def z_flows(links, zs, zr, sems, slot, tile):
    cols = lane_ds(tile)
    dst = [zr.at[slot, side, :, :, cols] for side in range(2)]
    return links.pair('gz', zs.at[0, :, :, cols], zs.at[1, :, :, cols], dst, sems, slot, tile)


def dot(a, b):
    return jnp.dot(a, b, preferred_element_type=F32)


def x_stage(src, xh, wx, me, layer, slot, tile, outer, edge, before_edge, emit):
    ny, nz, lanes = src.shape
    count = 8
    far, near = lanes - 2 * TILE, 0

    def rows(y, lane, width, weight):
        block = src[pl.ds(y, count), :, pl.ds(pl.multiple_of(lane, TILE), width)]
        return dot(block.reshape(count * nz, width), weight)

    @pl.when(outer)
    def _():
        weight = wx[layer, pl.ds(pl.multiple_of((1 - me) * TILE, TILE), 2 * TILE), :]
        for y in range(0, ny, count):
            emit(y, count, rows(y, me * far, 2 * TILE, weight))

    @pl.when(jnp.logical_not(outer | edge))
    def _():
        weight = wx[layer]
        for y in range(0, ny, count):
            emit(y, count, rows(y, (tile - 1) * TILE, 3 * TILE, weight))

    @pl.when(edge)
    def _():
        before_edge()
        weight = wx[layer, pl.ds(pl.multiple_of(me * TILE, TILE), 2 * TILE), :]
        other = wx[layer, pl.ds(pl.multiple_of((1 - me) * 2 * TILE, TILE), TILE), :]
        for y in range(0, ny, count):
            outside = dot(xh[slot, pl.ds(y, count)].reshape(count * nz, TILE), other)
            emit(y, count, rows(y, (1 - me) * far, 2 * TILE, weight) + outside)


def y_stage(src, halos, ly, layer, slot, tile, picks, emit):
    ny, nz, lanes, tiles, group, ysub = dims(src.shape, halos.shape[2])
    half = halos.shape[2]
    cols = lane_ds(tile)
    main = group * ROWS
    base = ly[layer, pl.ds(0, main), :]
    low = ly[layer, pl.ds(0, main + 2 * ROWS), :]
    high = jnp.concatenate([base, ly[layer, pl.ds(main + 2 * ROWS, 2 * ROWS), :]], axis=0)
    for g in range(ny // group):
        for zb in range(nz // ROWS):
            zrows = pl.ds(zb * ROWS, ROWS)
            first, last = g * group - half, g * group - half + ROWS
            parts = []
            if first < 0:
                parts.append(halos[slot, 0, :, zrows, cols])
            parts.append(src[pl.ds(max(first, 0), min(last, ny) - max(first, 0)), zrows, cols])
            if last > ny:
                parts.append(halos[slot, 1, :, zrows, cols])
            rhs = jnp.concatenate(parts, axis=0) if len(parts) > 1 else parts[0]
            side = {0: 0, nz // ROWS - 1: 1}.get(zb) if picks else None
            lhs = {None: base, 0: low, 1: high}[side]
            emit(g, zb, side, dot(lhs, rhs.reshape(ROWS * ROWS, TILE)).astype(BF16))


def z_stage(src, zr, lz, layer, slot, tile, ysub, emit):
    ny, nz, lanes = src.shape
    cols = lane_ds(tile)
    lhs = lz[layer]
    for g in range(ny // ysub):
        main = src[pl.ds(g * ysub, ysub), :, cols].reshape(ysub * nz, TILE)
        rhs = jnp.concatenate([main, zr[slot, 0, g, :, cols], zr[slot, 1, g, :, cols]], axis=0)
        emit(g, dot(lhs, rhs).astype(BF16).reshape(ysub, nz, TILE))


def fwd_kernel(half, sizes, v_hbm, cot_hbm, wx, ly, lz, wd, bias, a3_hbm, g_hbm, cbuf, crow, gbuf, cin_sem, gout_sem, vol, xh, a1, yr, a2, zs, zr, a3, in_sem, out_sem, xsend, xrecv, ysend, yrecv, zsend, zrecv):
    ny, nz, lanes, tiles, group, ysub = dims(v_hbm.shape, half)
    layers = wx.shape[0]
    links = Links(sizes)
    me = links.pos['gx']
    ysems, zsems, xsems = (ysend, yrecv), (zsend, zrecv), (xsend, xrecv)
    total = layers * tiles
    lag_y, lag_z = 2, 4
    assert lag_z <= tiles - 2

    def place(item):
        layer, p = item // tiles, lax.rem(item, tiles)
        return layer, p, p + me * (tiles - 1 - 2 * p), lax.rem(layer, 2)

    def fetch(tile):
        return pltpu.make_async_copy(v_hbm.at[:, :, lane_ds(tile)], vol.at[:, :, lane_ds(tile)], in_sem.at[tile])

    def put(layer, tile):
        return pltpu.make_async_copy(a3.at[:, :, lane_ds(tile)], a3_hbm.at[layer, :, :, lane_ds(tile)], out_sem.at[tile])

    def y_at(slot, tile):
        return y_flows(links, a1, yr, ysems, slot, tile)

    def z_at(slot, tile):
        return z_flows(links, zs, zr, zsems, slot, tile)

    def x_at(slot):
        return links.x_edge(vol, xh, xsems, slot, lanes)

    chans = cot_hbm.shape[0]
    per, sub = TILE // chans, ny // layers

    def cot_in(item):
        j, q = item // layers, lax.rem(item, layers)
        return pltpu.make_async_copy(cot_hbm.at[:, pl.ds(j * per, per), pl.ds(pl.multiple_of(q * sub, SUB), sub), :], cbuf.at[lax.rem(item, 2)], cin_sem.at[lax.rem(item, 2)])

    def cot_out(item):
        j, q = item // layers, lax.rem(item, layers)
        return pltpu.make_async_copy(gbuf.at[lax.rem(item, 2)], g_hbm.at[pl.ds(q * sub, sub), :, lane_ds(j)], gout_sem.at[lax.rem(item, 2)])

    edge_tile = place(tiles - 1)[2]
    fetch(edge_tile).start()
    for p in range(tiles - 1):
        fetch(place(p)[2]).start()
    cot_in(0).start()
    links.zero_edges('gy', yr)
    links.zero_edges('gz', zr)
    links.barrier()
    fetch(edge_tile).wait()
    x_at(0).start()

    @pl.loop(0, total + lag_z)
    def _(step):
        @pl.when(step < total)
        def _():
            layer, p, tile, slot = place(step)

            @pl.when(layer == 0)
            def _():
                pl.when(p == 0)(fetch(tile).wait)
                pl.when(p < tiles - 2)(fetch(place(p + 1)[2]).wait)

            @pl.when(layer > 0)
            def _():
                links.wait_send(y_at(1 - slot, tile))

            def before_edge():
                x_at(slot).wait_recv()
                x_at(slot).wait_send()

            def emit(y, count, out):
                a1[pl.ds(y, count), :, lane_ds(tile)] = out.astype(BF16).reshape(count, nz, TILE)

            x_stage(vol, xh, wx, me, layer, slot, tile, p == 0, p == tiles - 1, before_edge, emit)
            links.start(y_at(slot, tile))

        @pl.when((step >= lag_y) & (step < total + lag_y))
        def _():
            layer, p, tile, slot = place(step - lag_y)
            cols = lane_ds(tile)

            @pl.when(layer > 0)
            def _():
                links.wait_send(z_at(1 - slot, tile))

            links.wait_recv(y_at(slot, tile))

            def emit(g, zb, side, out):
                a2[pl.ds(g * group, group), pl.ds(zb * ROWS, ROWS), cols] = out[: group * ROWS].reshape(group, ROWS, TILE)
                if side is not None:
                    zs[side, pl.ds(2 * g, 2), :, cols] = out[group * ROWS :].reshape(2, ROWS, TILE)

            y_stage(a1, yr, ly, layer, slot, tile, True, emit)
            links.start(z_at(slot, tile))

        @pl.when(step >= lag_z)
        def _():
            layer, p, tile, slot = place(step - lag_z)
            cols = lane_ds(tile)

            @pl.when(layer > 0)
            def _():
                put(layer - 1, tile).wait()

            links.wait_recv(z_at(slot, tile))

            groups = ny // ysub

            def emit(g, out):
                a3[pl.ds(g * ysub, ysub), :, cols] = out

            @pl.when(layer == layers - 1)
            def _():
                z_stage(a2, zr, lz, layer, slot, tile, ysub, emit)

            @pl.when(layer < layers - 1)
            def _():
                held = {}

                def mix_and_update(g, out):
                    if out is not None:
                        emit(g, out)
                        held[g] = dot(out.reshape(ysub * nz, TILE), wd[layer])
                    if g >= 1:
                        mix = held.pop(g - 1)
                        for i in range(ysub):
                            y = (g - 1) * ysub + i
                            pre = mix[i * nz : (i + 1) * nz] + bias[layer]
                            new = vol[y, :, cols].astype(F32) + (0.5 * pre) * (1.0 + lax.erf(pre * INV_SQRT2))
                            vol[y, :, cols] = new.astype(BF16)

                z_stage(a2, zr, lz, layer, slot, tile, ysub, mix_and_update)
                mix_and_update(groups, None)
                pl.when(p == tiles - 1)(x_at(1 - slot).start)

            put(layer, tile).start()

        @pl.when(step < total)
        def _():
            slot = lax.rem(step, 2)
            cot_in(step).wait()
            pl.when(step + 1 < total)(cot_in(step + 1).start)
            pl.when(step >= 2)(cot_out(step - 2).wait)
            relayout(cbuf.at[slot], gbuf.at[slot], crow)
            cot_out(step).start()

    cot_out(total - 2).wait()
    cot_out(total - 1).wait()

    @pl.loop(0, tiles)
    def _(tile):
        slot = (layers - 1) % 2
        links.wait_send(y_at(slot, tile))
        links.wait_send(z_at(slot, tile))
        put(layers - 1, tile).wait()


def bwd_kernel(half, sizes, chans, a3_hbm, g_hbm, wx, ly, lz, pick, wd, wt, bias, go_hbm, sums, acts, grad, sb, d3, zs, zr, d2, yr, d1, xh, dw, db, gathered, act_sem, in_sem, out_sem, gsend, grecv, xsend, xrecv, ysend, yrecv, zsend, zrecv):
    ny, nz, lanes, tiles, group, ysub = dims(g_hbm.shape, half)
    layers = wx.shape[0]
    links = Links(sizes)
    me = links.pos['gx']
    ysems, zsems, xsems = (ysend, yrecv), (zsend, zrecv), (xsend, xrecv)
    total = layers * tiles
    lag_z, lag_y, lag_x = 2, 5, 6
    ahead = acts.shape[0] - 1
    assert lag_x <= tiles

    def place(item):
        turn, p = item // tiles, lax.rem(item, tiles)
        tile = (tiles - 1 - p) + me * (2 * p - tiles + 1)
        return layers - 1 - turn, turn, p, tile, lax.rem(turn, 2)

    def fetch(item):
        layer, turn, p, tile, slot = place(item)
        ring = lax.rem(item, ahead + 1)
        return pltpu.make_async_copy(a3_hbm.at[layer, :, :, lane_ds(tile)], acts.at[ring], act_sem.at[ring])

    def load(tile):
        return pltpu.make_async_copy(g_hbm.at[:, :, lane_ds(tile)], grad.at[:, :, lane_ds(tile)], in_sem.at[tile])

    def put(tile):
        return pltpu.make_async_copy(grad.at[:, :, lane_ds(tile)], go_hbm.at[:, :, lane_ds(tile)], out_sem.at[tile])

    def y_at(slot, tile):
        return y_flows(links, d2, yr, ysems, slot, tile)

    def z_at(slot, tile):
        return z_flows(links, zs, zr, zsems, slot, tile)

    def x_at(slot):
        return links.x_edge(d1, xh, xsems, slot, lanes)

    rounds = []
    for name, size in sizes.items():
        bit = 1
        while bit < size:
            rounds.append((name, bit))
            bit *= 2
    assert len(rounds) <= lag_x

    def share(index):
        name, bit = rounds[index]
        pos = links.pos[name]
        other = pos + bit - 2 * bit * lax.rem(pos // bit, 2)
        return pltpu.make_async_remote_copy(sums, gathered.at[index], gsend.at[index], grecv.at[index], device_id={name: other}, device_id_type=MESH)

    def finish(index):
        share(index).wait_send()
        share(index).wait_recv()
        sums[...] = sums[...] + gathered[index]

    for item in range(ahead):
        fetch(item).start()
        load(place(item)[3]).start()
    for item in range(ahead, tiles):
        load(place(item)[3]).start()
    links.zero_edges('gy', yr)
    links.zero_edges('gz', zr)
    links.barrier()

    @pl.loop(0, total + lag_x)
    def _(step):
        @pl.when((step >= lag_y) & (step < total + lag_y))
        def _():
            layer, turn, p, tile, slot = place(step - lag_y)
            cols = lane_ds(tile)
            links.wait_recv(y_at(slot, tile))

            def emit(g, zb, side, out):
                d1[pl.ds(g * group, group), pl.ds(zb * ROWS, ROWS), cols] = out.reshape(group, ROWS, TILE)

            y_stage(d2, yr, ly, layer, slot, tile, False, emit)
            pl.when(p == 0)(x_at(slot).start)

        @pl.when(step >= lag_x)
        def _():
            layer, turn, p, tile, slot = place(step - lag_x)
            cols = lane_ds(tile)

            def before_edge():
                x_at(slot).wait_recv()
                x_at(slot).wait_send()

            def emit(y, count, out):
                rows = pl.ds(y, count)
                old = grad[rows, :, cols].astype(F32).reshape(count * nz, TILE)
                grad[rows, :, cols] = (old + out).astype(BF16).reshape(count, nz, TILE)

            x_stage(d1, xh, wx, me, layer, slot, tile, p == tiles - 1, p == 0, before_edge, emit)
            pl.when(layer == 0)(put(tile).start)

        @pl.when(step < total)
        def _():
            layer, turn, p, tile, slot = place(step)
            cols = lane_ds(tile)
            ring = lax.rem(step, ahead + 1)
            fetch(step).wait()

            @pl.when(step + ahead < total)
            def _():
                fetch(step + ahead).start()

            @pl.when(turn == 0)
            def _():
                load(tile).wait()

            @pl.when(turn > 0)
            def _():
                links.wait_send(z_at(1 - slot, tile))

            @pl.when(p == 0)
            def _():
                dw[...] = jnp.zeros_like(dw)
                db[...] = jnp.zeros_like(db)

            span = ysub * nz
            groups = ny // ysub

            def mix_of(g):
                return dot(acts[ring, pl.ds(g * ysub, ysub)].reshape(span, TILE), wd[layer])

            totals = jnp.zeros((8, TILE), F32)
            mix, mixed = mix_of(0), {}
            for g in range(groups + 2):
                following = mix_of(g + 1) if g + 1 < groups else None
                if 1 <= g <= groups:
                    mixed[g - 1] = dot(sb[pl.ds((g - 1) * span, span), :], wt[layer]).astype(BF16)
                    d3[pl.ds((g - 1) * ysub, ysub), :, cols] = mixed[g - 1].reshape(ysub, nz, TILE)
                if g >= 2:
                    planes = dot(pick[...], mixed.pop(g - 2)).astype(BF16)
                    zs[0, g - 2, :, cols] = planes[:ROWS]
                    zs[1, g - 2, :, cols] = planes[ROWS:]
                if g < groups:
                    for i in range(ysub):
                        y = g * ysub + i
                        pre = mix[i * nz : (i + 1) * nz] + bias[layer]
                        cot = grad[y, :, cols].astype(F32)
                        root = pre * INV_SQRT2
                        bell = jnp.exp2((root * root) * NEG_LOG2E)
                        scaled = (0.5 * cot) * ((1.0 + lax.erf(root)) + (root * TWO_INV_SQRT_PI) * bell)
                        totals = totals + jnp.sum(scaled.reshape(nz // 8, 8, TILE), axis=0)
                        sb[pl.ds(y * nz, nz), :] = scaled.astype(BF16)
                mix = following
            db[...] += totals
            links.start(z_at(slot, tile))
            dw[...] += lax.dot_general(acts[ring].reshape(ny * nz, TILE), sb[...], (((0,), (0,)), ((), ())), preferred_element_type=F32)

            @pl.when(p == tiles - 1)
            def _():
                lane = lax.broadcasted_iota(jnp.int32, (chans, TILE), 1) // chans
                diag = jnp.zeros((chans, TILE), F32)
                for i in range(TILE // chans):
                    diag = diag + jnp.where(lane == i, dw[pl.ds(i * chans, chans), :], 0.0)
                sums[layer, pl.ds(0, chans), :] = diag
                sums[layer, pl.ds(chans, 8), :] = db[...]

        @pl.when((step >= lag_z) & (step < total + lag_z))
        def _():
            layer, turn, p, tile, slot = place(step - lag_z)
            cols = lane_ds(tile)

            @pl.when(turn > 0)
            def _():
                links.wait_send(y_at(1 - slot, tile))

            links.wait_recv(z_at(slot, tile))

            def emit(g, out):
                d2[pl.ds(g * ysub, ysub), :, cols] = out

            z_stage(d3, zr, lz, layer, slot, tile, ysub, emit)
            links.start(y_at(slot, tile))

        for index in range(len(rounds)):
            @pl.when(step == total + index)
            def _():
                if index > 0:
                    finish(index - 1)
                share(index).start()

    finish(len(rounds) - 1)

    @pl.loop(0, tiles)
    def _(tile):
        slot = (layers - 1) % 2
        links.wait_send(y_at(slot, tile))
        links.wait_send(z_at(slot, tile))
        put(tile).wait()


def link_sems(tiles):
    dma = pltpu.SemaphoreType.DMA
    return [dma, dma((2,)), dma((2, tiles)), dma((2, 2, tiles)), dma((2, tiles)), dma((2, 2, tiles))]


def solution(mesh):
    names = ('gx', 'gy', 'gz')
    sizes = {name: mesh.shape[name] for name in names}
    vol_spec = P('dp', 'gx', 'gy', 'gz')
    any_spec = pl.BlockSpec(memory_space=pl.ANY)
    vmem_spec = pl.BlockSpec(memory_space=pltpu.VMEM)
    dma = pltpu.SemaphoreType.DMA

    def local_step(volume, cot_out, filter_taps, w_mix, b_mix):
        chans, nx, ny, nz = volume.shape
        layers, _, num_taps = filter_taps.shape
        half = (num_taps - 1) // 2
        lanes = nx * chans
        tiles = lanes // TILE
        reps = TILE // chans
        ysub = (ROWS - 2 * half) // 2
        params = functools.partial(pltpu.CompilerParams, has_side_effects=True, vmem_limit_bytes=VMEM_BYTES)
        wx_f, wx_b, ly_f, ly_b, lz_f, lz_b, wd, wt = band_weights(filter_taps, w_mix, ysub, nz)
        pick = pick_matrix(half, ysub, nz)
        bias = jnp.tile(b_mix, (1, reps))[:, None, :]

        full = pltpu.VMEM((ny, nz, lanes), BF16)
        one = (ny, nz, TILE)
        two = pltpu.VMEM((2,) + one, BF16)
        y_halo = pltpu.VMEM((2, 2, half, nz, lanes), BF16)
        z_send = pltpu.VMEM((2, ny // ysub, ROWS, lanes), BF16)
        z_halo = pltpu.VMEM((2, 2, ny // ysub, ROWS, lanes), BF16)

        per, sub = TILE // chans, ny // layers
        acts, cot = pl.pallas_call(
            functools.partial(fwd_kernel, half, sizes),
            out_shape=[jax.ShapeDtypeStruct((layers, ny, nz, lanes), BF16), jax.ShapeDtypeStruct((ny, nz, lanes), BF16)],
            in_specs=[any_spec] * 2 + [vmem_spec] * 5,
            out_specs=[any_spec] * 2,
            scratch_shapes=[pltpu.VMEM((2, chans, per, sub, nz), BF16), pltpu.VMEM((TILE * (sub + SUB), nz), F32), pltpu.VMEM((2, sub, nz, TILE), BF16), dma((2,)), dma((2,))]
            + [full, two, full, y_halo, full, z_send, z_halo, full, dma((tiles,)), dma((tiles,))]
            + link_sems(tiles),
            compiler_params=params(collective_id=0),
            name='fwd_layers',
        )(to_dense(volume), cot_out, wx_f, ly_f, lz_f, wd, bias)
        rounds = sum((size - 1).bit_length() for size in sizes.values())
        sum_shape = (layers, chans + 8, TILE)
        grad, sums = pl.pallas_call(
            functools.partial(bwd_kernel, half, sizes, chans),
            out_shape=[jax.ShapeDtypeStruct((ny, nz, lanes), BF16), jax.ShapeDtypeStruct(sum_shape, F32)],
            in_specs=[any_spec] * 2 + [vmem_spec] * 7,
            out_specs=[any_spec, vmem_spec],
            scratch_shapes=[pltpu.VMEM((3,) + one, BF16), full, pltpu.VMEM((ny * nz, TILE), BF16), full, z_send, z_halo, full, y_halo, full, two]
            + [pltpu.VMEM((TILE, TILE), F32), pltpu.VMEM((8, TILE), F32), pltpu.VMEM((rounds,) + sum_shape, F32)]
            + [dma((3,)), dma((tiles,)), dma((tiles,)), dma((rounds,)), dma((rounds,))]
            + link_sems(tiles),
            compiler_params=params(collective_id=1),
            name='bwd_layers',
        )(acts, cot, wx_b, ly_b, lz_b, pick, wd, wt, bias)
        blocks = sums.reshape(layers, chans + 8, reps, chans).sum(axis=2)
        return from_dense(grad, chans), blocks[:, :chans], blocks[:, chans:].sum(axis=1)

    return jax.shard_map(local_step, mesh=mesh, in_specs=(vol_spec, vol_spec, P(), P(), P()), out_specs=(vol_spec, P('dp'), P('dp')), check_vma=False)
```

```python
import functools

import jax
import jax.numpy as jnp
import numpy as np
from jax import lax
from jax.experimental import pallas as pl
from jax.experimental.pallas import tpu as pltpu
from jax.sharding import PartitionSpec as P

MESH = pl.DeviceIdType.MESH
TILE = 256
ROWS = 16
LANE = 128
SUB = 8
VMEM_BYTES = 60 * 1024 * 1024
INV_SQRT2 = 0.7071067811865476
NEG_LOG2E = -1.4426950408889634
TWO_INV_SQRT_PI = 1.1283791670955126
F32 = jnp.float32
BF16 = jnp.bfloat16


def valid_index(index, keep, num_taps):
    return np.where(keep & (index >= 0) & (index < num_taps), index, -1).astype(np.int32)


def grid2(rows, cols):
    return np.arange(rows)[:, None], np.arange(cols)[None, :]


def x_index(num_taps, chans):
    x, n = grid2(3 * TILE // chans, TILE)
    index = x - TILE // chans - n // chans + num_taps // 2
    return valid_index(index, n >= 0, num_taps)


def y_index(num_taps):
    half = num_taps // 2
    group = ROWS - 2 * half
    r, k = grid2(group * ROWS, ROWS * ROWS)
    yi, zi = k // ROWS, k % ROWS
    parts = [valid_index(yi - r // ROWS, r % ROWS == zi, num_taps)]
    r, k = grid2(2 * ROWS, ROWS * ROWS)
    q = r % ROWS
    yo = r // ROWS * (group // 2) + q // half
    for first in (0, ROWS - half):
        keep = (q % half + first == zi) & (q < (group // 2) * half)
        parts.append(valid_index(yi - yo, keep, num_taps))
    return np.concatenate(parts, axis=0)


def z_index(num_taps, ysub, nz):
    half = num_taps // 2
    r, k = grid2(ysub * nz, ysub * nz + 2 * ROWS)
    yo, zo = r // nz, r % nz
    is_main = k < ysub * nz
    q = (k - ysub * nz) % ROWS
    low = k < ysub * nz + ROWS
    yi = np.where(is_main, k // nz, q // half)
    zi = np.where(is_main, k % nz, np.where(low, q % half - half, nz + q % half))
    keep = (yi == yo) & (is_main | (q < ysub * half))
    return valid_index(zi - zo + half, keep, num_taps)


def pick_matrix(half, ysub, nz):
    r, k = grid2(2 * ROWS, ysub * nz)
    q = r % ROWS
    zo = q % half + np.where(r < ROWS, 0, nz - half)
    hit = (k // nz == q // half) & (k % nz == zo) & (q < ysub * half)
    return jnp.asarray(hit, BF16)


def band_kernel(taps, wmix, bmix, spread, same, xi, yi, zi, xf, xb, yf, yb, zf, zb, wd, wt, bias):
    layers, _, num_taps = taps.shape
    chans = spread.shape[0]
    reps = TILE // chans

    def values(which, axis):
        zero = jnp.zeros(which.shape, F32)
        fwd, bwd = [zero] * layers, [zero] * layers
        for t in range(num_taps):
            hit = which == t
            for layer in range(layers):
                fwd[layer] = jnp.where(hit, taps[layer, axis, t], fwd[layer])
                bwd[layer] = jnp.where(hit, taps[layer, axis, num_taps - 1 - t], bwd[layer])
        return fwd, bwd

    diag = lax.rem(lax.broadcasted_iota(jnp.int32, (chans, TILE), 1), chans) == lax.broadcasted_iota(jnp.int32, (chans, TILE), 0)
    for dst, lines in zip((xf, xb), values(xi[...], 0)):
        for layer in range(layers):
            for x in range(xi.shape[0]):
                line = jnp.broadcast_to(lines[layer][x : x + 1], (chans, TILE))
                dst[layer, pl.ds(x * chans, chans), :] = jnp.where(diag, line, 0.0).astype(BF16)
    for axis, index, fwd, bwd in ((1, yi, yf, yb), (2, zi, zf, zb)):
        @pl.loop(0, index.shape[0] // ROWS)
        def _(chunk):
            rows = pl.ds(pl.multiple_of(chunk * ROWS, ROWS), ROWS)
            out = values(index[rows, :], axis)
            for layer in range(layers):
                fwd[layer, rows, :] = out[0][layer].astype(BF16)
                bwd[layer, rows, :] = out[1][layer].astype(BF16)
    for layer in range(layers):
        bias[layer] = jnp.concatenate([bmix[pl.ds(layer, 1), :]] * reps, axis=1)
        for dst, axis in ((wd, 1), (wt, 0)):
            wide = lax.dot_general(wmix[layer], spread[...], (((axis,), (0,)), ((), ())), preferred_element_type=F32)
            full = jnp.concatenate([wide] * reps, axis=0)
            dst[layer] = jnp.where(same[...] != 0, full, 0.0).astype(BF16)


def band_weights(filter_taps, w_mix, b_mix, ysub, nz):
    layers, _, num_taps = filter_taps.shape
    chans = w_mix.shape[1]
    r, n = grid2(TILE, TILE)
    spread = jnp.asarray(r[:chans] == n % chans, BF16)
    same = jnp.asarray(r // chans == n // chans, jnp.int32)
    indices = [x_index(num_taps, chans), y_index(num_taps), z_index(num_taps, ysub, nz)]
    vmem_spec = pl.BlockSpec(memory_space=pltpu.VMEM)
    shapes = [(3 * TILE, TILE)] * 2 + [i.shape for i in indices[1:] for _ in range(2)] + [(TILE, TILE)] * 2
    return pl.pallas_call(
        band_kernel,
        out_shape=[jax.ShapeDtypeStruct((layers,) + shape, BF16) for shape in shapes] + [jax.ShapeDtypeStruct((layers, 1, TILE), F32)],
        in_specs=[pl.BlockSpec(memory_space=pltpu.SMEM)] + [vmem_spec] * 7,
        out_specs=[vmem_spec] * 9,
        name='band_weights',
    )(filter_taps, w_mix, b_mix, spread, same, *[jnp.asarray(i) for i in indices])


def relayout(src, dst, rows):
    chans, nx, ny, nz = src.shape
    step = ny + 1
    for c in range(chans):
        for x in range(nx):
            rows[pl.ds((x * chans + c) * step, ny), :] = src[c, x].astype(F32)
    eye = (lax.broadcasted_iota(jnp.int32, (nz, nz), 0) == lax.broadcasted_iota(jnp.int32, (nz, nz), 1)).astype(BF16)

    @pl.loop(0, ny // SUB)
    def _(part):
        for i in range(SUB):
            y = part * SUB + i
            block = rows[pl.ds(y, TILE, stride=step), :].astype(BF16)
            out = lax.dot_general(eye, block, (((1,), (1,)), ((), ())), preferred_element_type=F32)
            dst[y] = out.astype(BF16)


def to_dense(a):
    chans, nx, ny, nz = a.shape
    per = TILE // chans
    return pl.pallas_call(
        relayout,
        grid=(nx // per,),
        in_specs=[pl.BlockSpec((chans, per, ny, nz), lambda i: (0, i, 0, 0))],
        out_specs=pl.BlockSpec((ny, nz, TILE), lambda i: (0, 0, i)),
        out_shape=jax.ShapeDtypeStruct((ny, nz, nx * chans), BF16),
        scratch_shapes=[pltpu.VMEM((TILE * (ny + 1), nz), F32)],
        compiler_params=pltpu.CompilerParams(vmem_limit_bytes=VMEM_BYTES),
        name='to_dense',
    )(a)


def leave_kernel(src, dst, rows):
    ny, nz, _ = src.shape
    chans, nx = dst.shape[:2]
    step = ny + 1
    eye = (lax.broadcasted_iota(jnp.int32, (TILE, TILE), 0) == lax.broadcasted_iota(jnp.int32, (TILE, TILE), 1)).astype(BF16)
    pad = jnp.zeros((LANE - nz, TILE), BF16)

    @pl.loop(0, ny // SUB)
    def _(part):
        for i in range(0, SUB, 2):
            y = part * SUB + i
            block = jnp.concatenate([src[y], pad, src[y + 1], pad], axis=0)
            out = lax.dot_general(eye, block, (((1,), (1,)), ((), ())), preferred_element_type=F32)
            rows[pl.ds(y, TILE, stride=step), :] = out[:, :LANE]
            rows[pl.ds(y + 1, TILE, stride=step), :] = out[:, LANE:]

    for c in range(chans):
        for x in range(nx):
            dst[c, x] = rows[pl.ds((x * chans + c) * step, ny), :][:, :nz].astype(BF16)


def from_dense(a, chans):
    ny, nz, lanes = a.shape
    per = TILE // chans
    return pl.pallas_call(
        leave_kernel,
        grid=(lanes // TILE,),
        in_specs=[pl.BlockSpec((ny, nz, TILE), lambda i: (0, 0, i))],
        out_specs=pl.BlockSpec((chans, per, ny, nz), lambda i: (0, i, 0, 0)),
        out_shape=jax.ShapeDtypeStruct((chans, lanes // chans, ny, nz), BF16),
        scratch_shapes=[pltpu.VMEM((TILE * (ny + 1), LANE), F32)],
        compiler_params=pltpu.CompilerParams(vmem_limit_bytes=VMEM_BYTES),
        name='from_dense',
    )(a)


def dims(shape, half):
    ny, nz, lanes = shape
    group = ROWS - 2 * half
    return ny, nz, lanes, lanes // TILE, group, group // 2


def lane_ds(tile):
    return pl.ds(pl.multiple_of(tile * TILE, TILE), TILE)


class Links:
    def __init__(self, sizes):
        self.sizes = sizes
        self.pos = {name: lax.axis_index(name) for name in ('gx', 'gy', 'gz')}

    def barrier(self):
        sem = pltpu.get_barrier_semaphore()
        count = 0
        for name, size in self.sizes.items():
            for step in range(1, size):
                pl.semaphore_signal(sem, inc=1, device_id={name: lax.rem(self.pos[name] + step, size)}, device_id_type=MESH)
                count += 1
        pl.semaphore_wait(sem, count)

    def pair(self, name, low_src, high_src, dst, sems, slot, tile):
        send, recv = sems
        pos, size = self.pos[name], self.sizes[name]
        down = pltpu.make_async_remote_copy(low_src, dst[1], send.at[0, tile], recv.at[slot, 0, tile], device_id={name: jnp.maximum(pos - 1, 0)}, device_id_type=MESH)
        up = pltpu.make_async_remote_copy(high_src, dst[0], send.at[1, tile], recv.at[slot, 1, tile], device_id={name: jnp.minimum(pos + 1, size - 1)}, device_id_type=MESH)
        return (down, pos > 0), (up, pos < size - 1)

    def start(self, flows):
        for copy, has in flows:
            pl.when(has)(copy.start)

    def wait_recv(self, flows):
        (down, has_low), (up, has_high) = flows
        pl.when(has_high)(down.wait_recv)
        pl.when(has_low)(up.wait_recv)

    def wait_send(self, flows):
        for copy, has in flows:
            pl.when(has)(copy.wait_send)

    def zero_edges(self, name, halos):
        for side, at in ((0, 0), (1, self.sizes[name] - 1)):
            @pl.when(self.pos[name] == at)
            def _():
                for slot in range(2):
                    halos[slot, side] = jnp.zeros(halos.shape[2:], halos.dtype)

    def x_edge(self, src, xh, sems, slot, lanes):
        send, recv = sems
        me = self.pos['gx']
        first = pl.multiple_of((1 - me) * (lanes - TILE), TILE)
        return pltpu.make_async_remote_copy(src.at[:, :, pl.ds(first, TILE)], xh.at[slot], send, recv.at[slot], device_id={'gx': 1 - me}, device_id_type=MESH)


def y_flows(links, buf, halos, sems, slot, tile):
    cols = lane_ds(tile)
    ny, half = buf.shape[0], halos.shape[2]
    dst = [halos.at[slot, side, :, :, cols] for side in range(2)]
    return links.pair('gy', buf.at[pl.ds(0, half), :, cols], buf.at[pl.ds(ny - half, half), :, cols], dst, sems, slot, tile)


def z_flows(links, zs, zr, sems, slot, tile):
    cols = lane_ds(tile)
    dst = [zr.at[slot, side, :, :, cols] for side in range(2)]
    return links.pair('gz', zs.at[0, :, :, cols], zs.at[1, :, :, cols], dst, sems, slot, tile)


def dot(a, b):
    return jnp.dot(a, b, preferred_element_type=F32)


def x_stage(src, xh, wx, me, layer, slot, tile, outer, edge, before_edge, emit):
    ny, nz, lanes = src.shape
    count = 8
    far, near = lanes - 2 * TILE, 0

    def rows(y, lane, width, weight):
        block = src[pl.ds(y, count), :, pl.ds(pl.multiple_of(lane, TILE), width)]
        return dot(block.reshape(count * nz, width), weight)

    @pl.when(outer)
    def _():
        weight = wx[layer, pl.ds(pl.multiple_of((1 - me) * TILE, TILE), 2 * TILE), :]
        for y in range(0, ny, count):
            emit(y, count, rows(y, me * far, 2 * TILE, weight))

    @pl.when(jnp.logical_not(outer | edge))
    def _():
        weight = wx[layer]
        for y in range(0, ny, count):
            emit(y, count, rows(y, (tile - 1) * TILE, 3 * TILE, weight))

    @pl.when(edge)
    def _():
        before_edge()
        weight = wx[layer, pl.ds(pl.multiple_of(me * TILE, TILE), 2 * TILE), :]
        other = wx[layer, pl.ds(pl.multiple_of((1 - me) * 2 * TILE, TILE), TILE), :]
        for y in range(0, ny, count):
            outside = dot(xh[slot, pl.ds(y, count)].reshape(count * nz, TILE), other)
            emit(y, count, rows(y, (1 - me) * far, 2 * TILE, weight) + outside)


def y_stage(src, halos, ly, layer, slot, tile, picks, emit):
    ny, nz, lanes, tiles, group, ysub = dims(src.shape, halos.shape[2])
    half = halos.shape[2]
    cols = lane_ds(tile)
    main = group * ROWS
    base = ly[layer, pl.ds(0, main), :]
    low = ly[layer, pl.ds(0, main + 2 * ROWS), :]
    high = jnp.concatenate([base, ly[layer, pl.ds(main + 2 * ROWS, 2 * ROWS), :]], axis=0)
    for g in range(ny // group):
        for zb in range(nz // ROWS):
            zrows = pl.ds(zb * ROWS, ROWS)
            first, last = g * group - half, g * group - half + ROWS
            parts = []
            if first < 0:
                parts.append(halos[slot, 0, :, zrows, cols])
            parts.append(src[pl.ds(max(first, 0), min(last, ny) - max(first, 0)), zrows, cols])
            if last > ny:
                parts.append(halos[slot, 1, :, zrows, cols])
            rhs = jnp.concatenate(parts, axis=0) if len(parts) > 1 else parts[0]
            side = {0: 0, nz // ROWS - 1: 1}.get(zb) if picks else None
            lhs = {None: base, 0: low, 1: high}[side]
            emit(g, zb, side, dot(lhs, rhs.reshape(ROWS * ROWS, TILE)).astype(BF16))


def z_stage(src, zr, lz, layer, slot, tile, ysub, emit):
    ny, nz, lanes = src.shape
    cols = lane_ds(tile)
    lhs = lz[layer]
    for g in range(ny // ysub):
        main = src[pl.ds(g * ysub, ysub), :, cols].reshape(ysub * nz, TILE)
        rhs = jnp.concatenate([main, zr[slot, 0, g, :, cols], zr[slot, 1, g, :, cols]], axis=0)
        emit(g, dot(lhs, rhs).astype(BF16).reshape(ysub, nz, TILE))


def fwd_kernel(half, sizes, v_hbm, cot_hbm, wx, ly, lz, wd, bias, a3_hbm, g_hbm, cbuf, crow, gbuf, cin_sem, gout_sem, vol, xh, a1, yr, a2, zs, zr, a3, in_sem, out_sem, xsend, xrecv, ysend, yrecv, zsend, zrecv):
    ny, nz, lanes, tiles, group, ysub = dims(v_hbm.shape, half)
    layers = wx.shape[0]
    links = Links(sizes)
    me = links.pos['gx']
    ysems, zsems, xsems = (ysend, yrecv), (zsend, zrecv), (xsend, xrecv)
    total = layers * tiles
    lag_y, lag_z = 2, 4
    assert lag_z <= tiles - 2

    def place(item):
        layer, p = item // tiles, lax.rem(item, tiles)
        return layer, p, p + me * (tiles - 1 - 2 * p), lax.rem(layer, 2)

    def fetch(tile):
        return pltpu.make_async_copy(v_hbm.at[:, :, lane_ds(tile)], vol.at[:, :, lane_ds(tile)], in_sem.at[tile])

    def put(layer, tile):
        return pltpu.make_async_copy(a3.at[:, :, lane_ds(tile)], a3_hbm.at[layer, :, :, lane_ds(tile)], out_sem.at[tile])

    def y_at(slot, tile):
        return y_flows(links, a1, yr, ysems, slot, tile)

    def z_at(slot, tile):
        return z_flows(links, zs, zr, zsems, slot, tile)

    def x_at(slot):
        return links.x_edge(vol, xh, xsems, slot, lanes)

    chans = cot_hbm.shape[0]
    per, sub = TILE // chans, ny // layers

    def cot_in(item):
        j, q = item // layers, lax.rem(item, layers)
        return pltpu.make_async_copy(cot_hbm.at[:, pl.ds(j * per, per), pl.ds(pl.multiple_of(q * sub, SUB), sub), :], cbuf.at[lax.rem(item, 2)], cin_sem.at[lax.rem(item, 2)])

    def cot_out(item):
        j, q = item // layers, lax.rem(item, layers)
        return pltpu.make_async_copy(gbuf.at[lax.rem(item, 2)], g_hbm.at[pl.ds(q * sub, sub), :, lane_ds(j)], gout_sem.at[lax.rem(item, 2)])

    edge_tile = place(tiles - 1)[2]
    fetch(edge_tile).start()
    for p in range(tiles - 1):
        fetch(place(p)[2]).start()
    cot_in(0).start()
    links.zero_edges('gy', yr)
    links.zero_edges('gz', zr)
    links.barrier()
    fetch(edge_tile).wait()
    x_at(0).start()

    @pl.loop(0, total + lag_z)
    def _(step):
        @pl.when(step < total)
        def _():
            layer, p, tile, slot = place(step)

            @pl.when(layer == 0)
            def _():
                pl.when(p == 0)(fetch(tile).wait)
                pl.when(p < tiles - 2)(fetch(place(p + 1)[2]).wait)

            @pl.when(layer > 0)
            def _():
                links.wait_send(y_at(1 - slot, tile))

            def before_edge():
                x_at(slot).wait_recv()
                x_at(slot).wait_send()

            def emit(y, count, out):
                a1[pl.ds(y, count), :, lane_ds(tile)] = out.astype(BF16).reshape(count, nz, TILE)

            x_stage(vol, xh, wx, me, layer, slot, tile, p == 0, p == tiles - 1, before_edge, emit)
            links.start(y_at(slot, tile))

        @pl.when((step >= lag_y) & (step < total + lag_y))
        def _():
            layer, p, tile, slot = place(step - lag_y)
            cols = lane_ds(tile)

            @pl.when(layer > 0)
            def _():
                links.wait_send(z_at(1 - slot, tile))

            links.wait_recv(y_at(slot, tile))

            def emit(g, zb, side, out):
                a2[pl.ds(g * group, group), pl.ds(zb * ROWS, ROWS), cols] = out[: group * ROWS].reshape(group, ROWS, TILE)
                if side is not None:
                    zs[side, pl.ds(2 * g, 2), :, cols] = out[group * ROWS :].reshape(2, ROWS, TILE)

            y_stage(a1, yr, ly, layer, slot, tile, True, emit)
            links.start(z_at(slot, tile))

        @pl.when(step >= lag_z)
        def _():
            layer, p, tile, slot = place(step - lag_z)
            cols = lane_ds(tile)

            @pl.when(layer > 0)
            def _():
                put(layer - 1, tile).wait()

            links.wait_recv(z_at(slot, tile))

            groups = ny // ysub

            def emit(g, out):
                a3[pl.ds(g * ysub, ysub), :, cols] = out

            @pl.when(layer == layers - 1)
            def _():
                z_stage(a2, zr, lz, layer, slot, tile, ysub, emit)

            @pl.when(layer < layers - 1)
            def _():
                held = {}

                def mix_and_update(g, out):
                    if out is not None:
                        emit(g, out)
                        held[g] = dot(out.reshape(ysub * nz, TILE), wd[layer])
                    if g >= 1:
                        mix = held.pop(g - 1)
                        for i in range(ysub):
                            y = (g - 1) * ysub + i
                            pre = mix[i * nz : (i + 1) * nz] + bias[layer]
                            new = vol[y, :, cols].astype(F32) + (0.5 * pre) * (1.0 + lax.erf(pre * INV_SQRT2))
                            vol[y, :, cols] = new.astype(BF16)

                z_stage(a2, zr, lz, layer, slot, tile, ysub, mix_and_update)
                mix_and_update(groups, None)
                pl.when(p == tiles - 1)(x_at(1 - slot).start)

            put(layer, tile).start()

        @pl.when(step < total)
        def _():
            slot = lax.rem(step, 2)
            cot_in(step).wait()
            pl.when(step + 1 < total)(cot_in(step + 1).start)
            pl.when(step >= 2)(cot_out(step - 2).wait)
            relayout(cbuf.at[slot], gbuf.at[slot], crow)
            cot_out(step).start()

    cot_out(total - 2).wait()
    cot_out(total - 1).wait()

    @pl.loop(0, tiles)
    def _(tile):
        slot = (layers - 1) % 2
        links.wait_send(y_at(slot, tile))
        links.wait_send(z_at(slot, tile))
        put(layers - 1, tile).wait()


def bwd_kernel(half, sizes, chans, a3_hbm, g_hbm, wx, ly, lz, pick, wd, wt, bias, go_hbm, sums, acts, grad, sb, d3, zs, zr, d2, yr, d1, xh, dw, db, gathered, act_sem, in_sem, out_sem, gsend, grecv, xsend, xrecv, ysend, yrecv, zsend, zrecv):
    ny, nz, lanes, tiles, group, ysub = dims(g_hbm.shape, half)
    layers = wx.shape[0]
    links = Links(sizes)
    me = links.pos['gx']
    ysems, zsems, xsems = (ysend, yrecv), (zsend, zrecv), (xsend, xrecv)
    total = layers * tiles
    lag_z, lag_y, lag_x = 2, 5, 6
    ahead = acts.shape[0] - 1
    assert lag_x <= tiles

    def place(item):
        turn, p = item // tiles, lax.rem(item, tiles)
        tile = (tiles - 1 - p) + me * (2 * p - tiles + 1)
        return layers - 1 - turn, turn, p, tile, lax.rem(turn, 2)

    def fetch(item):
        layer, turn, p, tile, slot = place(item)
        ring = lax.rem(item, ahead + 1)
        return pltpu.make_async_copy(a3_hbm.at[layer, :, :, lane_ds(tile)], acts.at[ring], act_sem.at[ring])

    def load(tile):
        return pltpu.make_async_copy(g_hbm.at[:, :, lane_ds(tile)], grad.at[:, :, lane_ds(tile)], in_sem.at[tile])

    def put(tile):
        return pltpu.make_async_copy(grad.at[:, :, lane_ds(tile)], go_hbm.at[:, :, lane_ds(tile)], out_sem.at[tile])

    def y_at(slot, tile):
        return y_flows(links, d2, yr, ysems, slot, tile)

    def z_at(slot, tile):
        return z_flows(links, zs, zr, zsems, slot, tile)

    def x_at(slot):
        return links.x_edge(d1, xh, xsems, slot, lanes)

    rounds = []
    for name, size in sizes.items():
        bit = 1
        while bit < size:
            rounds.append((name, bit))
            bit *= 2
    assert len(rounds) <= lag_x

    def share(index):
        name, bit = rounds[index]
        pos = links.pos[name]
        other = pos + bit - 2 * bit * lax.rem(pos // bit, 2)
        return pltpu.make_async_remote_copy(sums, gathered.at[index], gsend.at[index], grecv.at[index], device_id={name: other}, device_id_type=MESH)

    def finish(index):
        share(index).wait_send()
        share(index).wait_recv()
        sums[...] = sums[...] + gathered[index]

    for item in range(ahead):
        fetch(item).start()
        load(place(item)[3]).start()
    for item in range(ahead, tiles):
        load(place(item)[3]).start()
    links.zero_edges('gy', yr)
    links.zero_edges('gz', zr)
    links.barrier()

    @pl.loop(0, total + lag_x)
    def _(step):
        @pl.when((step >= lag_y) & (step < total + lag_y))
        def _():
            layer, turn, p, tile, slot = place(step - lag_y)
            cols = lane_ds(tile)
            links.wait_recv(y_at(slot, tile))

            def emit(g, zb, side, out):
                d1[pl.ds(g * group, group), pl.ds(zb * ROWS, ROWS), cols] = out.reshape(group, ROWS, TILE)

            y_stage(d2, yr, ly, layer, slot, tile, False, emit)
            pl.when(p == 0)(x_at(slot).start)

        @pl.when(step >= lag_x)
        def _():
            layer, turn, p, tile, slot = place(step - lag_x)
            cols = lane_ds(tile)

            def before_edge():
                x_at(slot).wait_recv()
                x_at(slot).wait_send()

            def emit(y, count, out):
                rows = pl.ds(y, count)
                old = grad[rows, :, cols].astype(F32).reshape(count * nz, TILE)
                grad[rows, :, cols] = (old + out).astype(BF16).reshape(count, nz, TILE)

            x_stage(d1, xh, wx, me, layer, slot, tile, p == tiles - 1, p == 0, before_edge, emit)
            pl.when(layer == 0)(put(tile).start)

        @pl.when(step < total)
        def _():
            layer, turn, p, tile, slot = place(step)
            cols = lane_ds(tile)
            ring = lax.rem(step, ahead + 1)
            fetch(step).wait()

            @pl.when(step + ahead < total)
            def _():
                fetch(step + ahead).start()

            @pl.when(turn == 0)
            def _():
                load(tile).wait()

            @pl.when(turn > 0)
            def _():
                links.wait_send(z_at(1 - slot, tile))

            @pl.when(p == 0)
            def _():
                dw[...] = jnp.zeros_like(dw)
                db[...] = jnp.zeros_like(db)

            span = ysub * nz
            groups = ny // ysub

            def mix_of(g):
                return dot(acts[ring, pl.ds(g * ysub, ysub)].reshape(span, TILE), wd[layer])

            totals = jnp.zeros((8, TILE), F32)
            mix, mixed = mix_of(0), {}
            for g in range(groups + 2):
                following = mix_of(g + 1) if g + 1 < groups else None
                if 1 <= g <= groups:
                    mixed[g - 1] = dot(sb[pl.ds((g - 1) * span, span), :], wt[layer]).astype(BF16)
                    d3[pl.ds((g - 1) * ysub, ysub), :, cols] = mixed[g - 1].reshape(ysub, nz, TILE)
                if g >= 2:
                    planes = dot(pick[...], mixed.pop(g - 2)).astype(BF16)
                    zs[0, g - 2, :, cols] = planes[:ROWS]
                    zs[1, g - 2, :, cols] = planes[ROWS:]
                if g < groups:
                    for i in range(ysub):
                        y = g * ysub + i
                        pre = mix[i * nz : (i + 1) * nz] + bias[layer]
                        cot = grad[y, :, cols].astype(F32)
                        root = pre * INV_SQRT2
                        bell = jnp.exp2((root * root) * NEG_LOG2E)
                        scaled = (0.5 * cot) * ((1.0 + lax.erf(root)) + (root * TWO_INV_SQRT_PI) * bell)
                        totals = totals + jnp.sum(scaled.reshape(nz // 8, 8, TILE), axis=0)
                        sb[pl.ds(y * nz, nz), :] = scaled.astype(BF16)
                mix = following
            db[...] += totals
            links.start(z_at(slot, tile))
            dw[...] += lax.dot_general(acts[ring].reshape(ny * nz, TILE), sb[...], (((0,), (0,)), ((), ())), preferred_element_type=F32)

            @pl.when(p == tiles - 1)
            def _():
                lane = lax.broadcasted_iota(jnp.int32, (chans, TILE), 1) // chans
                diag = jnp.zeros((chans, TILE), F32)
                for i in range(TILE // chans):
                    diag = diag + jnp.where(lane == i, dw[pl.ds(i * chans, chans), :], 0.0)
                sums[layer, pl.ds(0, chans), :] = diag
                sums[layer, pl.ds(chans, 8), :] = db[...]

        @pl.when((step >= lag_z) & (step < total + lag_z))
        def _():
            layer, turn, p, tile, slot = place(step - lag_z)
            cols = lane_ds(tile)

            @pl.when(turn > 0)
            def _():
                links.wait_send(y_at(1 - slot, tile))

            links.wait_recv(z_at(slot, tile))

            def emit(g, out):
                d2[pl.ds(g * ysub, ysub), :, cols] = out

            z_stage(d3, zr, lz, layer, slot, tile, ysub, emit)
            links.start(y_at(slot, tile))

        for index in range(len(rounds)):
            @pl.when(step == total + index)
            def _():
                if index > 0:
                    finish(index - 1)
                share(index).start()

    finish(len(rounds) - 1)

    @pl.loop(0, tiles)
    def _(tile):
        slot = (layers - 1) % 2
        links.wait_send(y_at(slot, tile))
        links.wait_send(z_at(slot, tile))
        put(tile).wait()


def link_sems(tiles):
    dma = pltpu.SemaphoreType.DMA
    return [dma, dma((2,)), dma((2, tiles)), dma((2, 2, tiles)), dma((2, tiles)), dma((2, 2, tiles))]


def solution(mesh):
    names = ('gx', 'gy', 'gz')
    sizes = {name: mesh.shape[name] for name in names}
    vol_spec = P('dp', 'gx', 'gy', 'gz')
    any_spec = pl.BlockSpec(memory_space=pl.ANY)
    vmem_spec = pl.BlockSpec(memory_space=pltpu.VMEM)
    dma = pltpu.SemaphoreType.DMA

    def local_step(volume, cot_out, filter_taps, w_mix, b_mix):
        chans, nx, ny, nz = volume.shape
        layers, _, num_taps = filter_taps.shape
        half = (num_taps - 1) // 2
        lanes = nx * chans
        tiles = lanes // TILE
        reps = TILE // chans
        ysub = (ROWS - 2 * half) // 2
        params = functools.partial(pltpu.CompilerParams, has_side_effects=True, vmem_limit_bytes=VMEM_BYTES)
        wx_f, wx_b, ly_f, ly_b, lz_f, lz_b, wd, wt, bias = band_weights(filter_taps, w_mix, b_mix, ysub, nz)
        pick = pick_matrix(half, ysub, nz)

        full = pltpu.VMEM((ny, nz, lanes), BF16)
        one = (ny, nz, TILE)
        two = pltpu.VMEM((2,) + one, BF16)
        y_halo = pltpu.VMEM((2, 2, half, nz, lanes), BF16)
        z_send = pltpu.VMEM((2, ny // ysub, ROWS, lanes), BF16)
        z_halo = pltpu.VMEM((2, 2, ny // ysub, ROWS, lanes), BF16)

        per, sub = TILE // chans, ny // layers
        acts, cot = pl.pallas_call(
            functools.partial(fwd_kernel, half, sizes),
            out_shape=[jax.ShapeDtypeStruct((layers, ny, nz, lanes), BF16), jax.ShapeDtypeStruct((ny, nz, lanes), BF16)],
            in_specs=[any_spec] * 2 + [vmem_spec] * 5,
            out_specs=[any_spec] * 2,
            scratch_shapes=[pltpu.VMEM((2, chans, per, sub, nz), BF16), pltpu.VMEM((TILE * (sub + 1), nz), F32), pltpu.VMEM((2, sub, nz, TILE), BF16), dma((2,)), dma((2,))]
            + [full, two, full, y_halo, full, z_send, z_halo, full, dma((tiles,)), dma((tiles,))]
            + link_sems(tiles),
            compiler_params=params(collective_id=0),
            name='fwd_layers',
        )(to_dense(volume), cot_out, wx_f, ly_f, lz_f, wd, bias)
        rounds = sum((size - 1).bit_length() for size in sizes.values())
        sum_shape = (layers, chans + 8, TILE)
        grad, sums = pl.pallas_call(
            functools.partial(bwd_kernel, half, sizes, chans),
            out_shape=[jax.ShapeDtypeStruct((ny, nz, lanes), BF16), jax.ShapeDtypeStruct(sum_shape, F32)],
            in_specs=[any_spec] * 2 + [vmem_spec] * 7,
            out_specs=[any_spec, vmem_spec],
            scratch_shapes=[pltpu.VMEM((3,) + one, BF16), full, pltpu.VMEM((ny * nz, TILE), BF16), full, z_send, z_halo, full, y_halo, full, two]
            + [pltpu.VMEM((TILE, TILE), F32), pltpu.VMEM((8, TILE), F32), pltpu.VMEM((rounds,) + sum_shape, F32)]
            + [dma((3,)), dma((tiles,)), dma((tiles,)), dma((rounds,)), dma((rounds,))]
            + link_sems(tiles),
            compiler_params=params(collective_id=1),
            name='bwd_layers',
        )(acts, cot, wx_b, ly_b, lz_b, pick, wd, wt, bias)
        blocks = sums.reshape(layers, chans + 8, reps, chans).sum(axis=2)
        return from_dense(grad, chans), blocks[:, :chans], blocks[:, chans:].sum(axis=1)

    return jax.shard_map(local_step, mesh=mesh, in_specs=(vol_spec, vol_spec, P(), P(), P()), out_specs=(vol_spec, P('dp'), P('dp')), check_vma=False)
```
